128 devices in a mesh: task: 8 (over x_hi, z), dp: 16 (over x_lo, y, core).
Axes of the slice: x: 4 (x_hi: 2, x_lo: 2; x = x_hi * 2 + x_lo), y: 4, z: 4, core: 2. Of those that a mesh axis runs over, the one named last changes fastest.
Arguments:
- tokens_in: bfloat16 [131072, 4096], P(('task', 'dp')), may hold values from -45 to 45
- query_cotangent: bfloat16 [131072, 2048], P(('task', 'dp')), may hold values from -23040 to 23040
- task_index: int32 [131072], P(('task', 'dp')), may hold values from 0 to 15, as said below
- loss_weights: int32 [16], replicated, may hold values from 1 to 4
- master: float32 [4096, 2048], P(('task', 'dp')), may hold values from -6 to 6
- moment_first: float32 [4096, 2048], P(('task', 'dp')), may hold values from -6 to 6
- moment_second: float32 [4096, 2048], P(('task', 'dp')), may hold values from 0.05 to 5
Outputs:
- new_master: float32 [4096, 2048], P(('task', 'dp'))
- new_first: float32 [4096, 2048], P(('task', 'dp'))
- new_second: float32 [4096, 2048], P(('task', 'dp'))
The draws below stay inside these ranges and needn't reach their ends.
Inputs may be any that keep to these rules, and one draw needn't show every extreme that they name: `task_index`: the first 16 tokens name each task once.
All inputs are finite; a program needn't handle non-finite values.
Results may differ from the reference program's by a relative error of at most 0.00042.
Values may be sent and summed in bfloat16 or wider, within the bound.
A program may use at most 192 MiB of HBM per device.

```python
import math
import jax
import jax.numpy as jnp
from jax import lax

D = 4096
QW = 2048
TASKS = 16
TOK_DEV = 1024
TOKENS = 131072
DEVICES = 128


def column_profile(key, col_count, spread):
    position = jnp.arange(col_count, dtype=jnp.float32) / col_count
    exponent = jax.random.uniform(key, (col_count,), jnp.float32)
    return 3.0 ** position * spread ** exponent


def field_values(key, row_count, col_count):
    subkeys = jax.random.split(key, 2)
    scales = column_profile(subkeys[0], col_count, 10.0)
    values = jnp.clip(jax.random.normal(subkeys[1], (row_count, col_count), jnp.float32), -6.0, 6.0)
    return values * scales[None, :] * 0.25


def draw_tokens_in(key, part):
    return field_values(jax.random.fold_in(key, 11), TOKENS, D).astype(jnp.bfloat16)


def draw_query_cotangent(key, part):
    amplitude = float(TOKENS // (TASKS * TASKS))
    inputs = field_values(jax.random.fold_in(key, 11), TOKENS, D)
    own_part = field_values(jax.random.fold_in(key, 23), TOKENS, QW)
    block_size = math.gcd(QW, 128)
    block_count = QW // block_size
    mixing = jax.random.normal(jax.random.fold_in(key, 29), (block_count, block_size, block_size), jnp.float32)
    mixing = mixing / math.sqrt(block_size)
    leading = inputs[:, :QW].reshape(TOKENS, block_count, block_size)
    carried = jnp.einsum('nbk,bkj->nbj', leading, mixing, precision=lax.Precision.HIGHEST)
    combined = jnp.clip(own_part + 0.15 * carried.reshape(TOKENS, QW), -45.0, 45.0)
    return (combined * amplitude).astype(jnp.bfloat16)


def draw_task_index(key, part):
    subkeys = jax.random.split(jax.random.fold_in(key, 37), 2)
    rows_all = jnp.arange(TOKENS, dtype=jnp.int32)
    shifted = rows_all * TASKS // TOKENS
    offsets = jax.random.randint(subkeys[0], (TOKENS,), 0, TASKS // 2, dtype=jnp.int32)
    sliding = (shifted + offsets) % TASKS
    ordering = jax.random.permutation(subkeys[1], jnp.arange(TASKS, dtype=jnp.int32))
    leading = ordering[jnp.minimum(rows_all, TASKS - 1)]
    return jnp.where(rows_all < TASKS, leading, sliding).astype(jnp.int32)


def set_ends(result, key, least, high):
    index_at = [jax.random.randint(jax.random.fold_in(key, axis), (), 0, length) for axis, length in enumerate(result.shape)]
    main_axis = result.shape.index(max(result.shape))
    neighbour = index_at[:main_axis] + [(index_at[main_axis] + 1) % result.shape[main_axis]] + index_at[main_axis + 1:]
    return result.at[tuple(index_at)].set(least).at[tuple(neighbour)].set(high)


def level_of(key, dims, shards, low, high):
    loudness = 1.0
    for dim, shards_of in shards:
        draws = jax.random.uniform(jax.random.fold_in(jax.random.fold_in(key, 6), dim), (shards_of,), jnp.float32, low / len(shards), high / len(shards))
        loudness = loudness * jnp.repeat(jnp.exp(draws), dims[dim] // shards_of).reshape((-1,) + (1,) * (len(dims) - 1 - dim))
    return loudness


def normal_values(stream_key, extent, width, limit, pieces=(), held_as=jnp.bfloat16):
    level = level_of(stream_key, extent, pieces, -0.22, 0.18) if pieces else 1.0
    array = jax.random.normal(stream_key, extent, jnp.float32) * width * level
    return jnp.minimum(jnp.maximum(array, -limit), limit).astype(held_as)


def setup_inputs(seed: int = 0) -> dict:
    key_of = jax.random.split(jax.random.key(seed), 8)
    tokens_in = draw_tokens_in(jax.random.fold_in(key_of[7], 71), 0)
    query_cotangent = draw_query_cotangent(jax.random.fold_in(key_of[7], 71), 0)
    task_index = draw_task_index(jax.random.fold_in(key_of[7], 71), 0)
    loss_weights = set_ends(jax.random.randint(key_of[3], (TASKS,), 1, 5), jax.random.fold_in(key_of[3], 1), 1, 4).astype(jnp.int32)
    master = normal_values(key_of[4], (D, QW), 1.0, 6.0, ((0, 128),), jnp.float32)
    moment_first = normal_values(key_of[5], (D, QW), 1.0, 6.0, ((0, 128),), jnp.float32)
    moment_second = jnp.clip(jnp.exp(math.log(5.0) - 4.6051702 * jax.random.uniform(key_of[6], (D, QW), jnp.float32) ** level_of(key_of[6], (D, QW), ((0, 128),), -0.2, 0.2)), 0.05, 5.0)
    return dict(tokens_in=tokens_in, query_cotangent=query_cotangent, task_index=task_index, loss_weights=loss_weights, master=master, moment_first=moment_first, moment_second=moment_second)


beta_one = 0.9
beta_two = 0.95
adam_eps = 1e-08
step_rate = 0.01
decay_rate = 0.1
corr_one = 1.0 - 0.9 ** 10
corr_two = 1.0 - 0.95 ** 10

def reference(tokens_in, query_cotangent, task_index, loss_weights, master, moment_first, moment_second):
    labels = jnp.arange(TASKS, dtype=jnp.int32)
    member = task_index[:, None] == labels[None, :]
    counts = lax.optimization_barrier(jnp.sum(member.astype(jnp.int32), axis=0))
    task_scale = loss_weights.astype(jnp.float32) / counts.astype(jnp.float32)
    token_scale = lax.optimization_barrier(jnp.sum(jnp.where(member, task_scale[None, :], jnp.float32(0.0)), axis=1))
    weighted = (query_cotangent.astype(jnp.float32) * token_scale[:, None]).astype(jnp.bfloat16)
    token_blocks = tokens_in.reshape(DEVICES, TOK_DEV, D)
    weight_blocks = weighted.reshape(DEVICES, TOK_DEV, QW)

    def add_block(running, blocks_pair):
        product = jnp.dot(blocks_pair[0].T, blocks_pair[1], preferred_element_type=jnp.float32)
        return (running + product, None)
    gradient, unused = lax.scan(add_block, jnp.zeros((D, QW), jnp.float32), (token_blocks, weight_blocks))
    square_sum = jnp.sum(gradient * gradient)
    root_mean = jnp.sqrt(square_sum / (D * QW))
    clip = 1.0 / jnp.maximum(root_mean, 1.0)
    clipped = gradient * clip
    new_first = beta_one * moment_first + (1.0 - beta_one) * clipped
    new_second = beta_two * moment_second + (1.0 - beta_two) * clipped * clipped
    direction = new_first / corr_one / (jnp.sqrt(new_second / corr_two) + adam_eps)
    new_master = master - step_rate * (direction + decay_rate * master)
    return (new_master, new_first, new_second)
```

```python
import jax
import jax.numpy as jnp
from jax import lax
from jax.experimental import pallas as pl
from jax.experimental.pallas import tpu as pltpu
from jax.sharding import Mesh
from jax.sharding import PartitionSpec as P

D = 4096
QW = 2048
TASKS = 16
AXES = ("task_0", "task_1", "dp_0", "dp_1", "dp_2")
MESH = pl.DeviceIdType.MESH

beta_one = 0.9
beta_two = 0.95
adam_eps = 1e-08
step_rate = 0.01
decay_rate = 0.1
corr_one = 1.0 - 0.9**10
corr_two = 1.0 - 0.95**10

TOK = 1024
HALF = QW // 2
C0, W0 = 0, 384
C1, W1 = 384, 384
C2, W2 = 768, 256
LAG = 3
DX = (2, 2, 0, 1, 2, 3, 2, 1, 1, 0, 3, 1, 3, 0, 3, 0)
DZ = (2, 0, 2, 2, 1, 2, 3, 1, 0, 1, 1, 3, 0, 3, 3, 0)
TOP = 32766.0


def pick(i, table):
    out = jnp.int32(table[0])
    for j in range(1, len(table)):
        out = jnp.where(i == j, jnp.int32(table[j]), out)
    return out


def tiles(rows, width):
    return (rows // 16) * (width // 128)


def encode(src, r0, rows, c0, width, msg):
    nc = width // 128

    def largest(t, m):
        for j in range(nc):
            a = jnp.abs(src[pl.ds(r0 + t * 16, 16), pl.ds(c0 + j * 128, 128)])
            m = jnp.maximum(m, jnp.maximum(a[:8], a[8:]))
        return m

    m = lax.fori_loop(0, rows // 16, largest, jnp.zeros((8, 128), jnp.float32), unroll=2)
    e = jnp.ceil(jnp.log2(jnp.maximum(m, 1e-30)) + 0.001)
    inv = jnp.exp2(-e) * TOP
    inv = jnp.concatenate([inv, inv], axis=0)

    def put(t, carry):
        for j in range(nc):
            v = src[pl.ds(r0 + t * 16, 16), pl.ds(c0 + j * 128, 128)]
            msg[t * nc + j] = jnp.round(v * inv).astype(jnp.int32).astype(jnp.int16)
        return carry

    lax.fori_loop(0, rows // 16, put, 0, unroll=2)
    msg[tiles(rows, width)] = jnp.concatenate([e, e], axis=0).astype(jnp.int32).astype(jnp.int16)


def decode_add(dst, r0, rows, c0, width, msg):
    nc = width // 128
    e = msg[tiles(rows, width)].astype(jnp.int32).astype(jnp.float32)
    scale = jnp.exp2(e) * (1.0 / TOP)

    def add(t, carry):
        for j in range(nc):
            at = (pl.ds(r0 + t * 16, 16), pl.ds(c0 + j * 128, 128))
            dst[at] = dst[at] + msg[t * nc + j].astype(jnp.int32).astype(jnp.float32) * scale
        return carry

    lax.fori_loop(0, rows // 16, add, 0, unroll=2)


def copy_rows(dst, dr0, src, sr0, rows, c0, width):
    def put(t, carry):
        for j in range(width // 128):
            dst[pl.ds(dr0 + t * 16, 16), pl.ds(j * 128, 128)] = src[
                pl.ds(sr0 + t * 16, 16), pl.ds(c0 + j * 128, 128)
            ]
        return carry

    lax.fori_loop(0, rows // 16, put, 0, unroll=2)


def kernel(
    tok_hbm, cot_hbm, idx_hbm, lw_smem, grad_ref, clip_ref,
    tok, w, idx, tsc, acc,
    own0, own1, own2, hold1,
    sA0, rA0, sB0, rB0,
    sA2, rA2, sB2, rB2,
    sA1, rA1, sB1, rB1,
    s2A, r2A, s2B, r2B, s2A2, r2A2, s2B2, r2B2,
    s3A, r3A, s3B, r3B, s3A2, r3A2, s3B2, r3B2,
    cnt1, cnt2, nrm1, nrm2, fin, finr,
    loc_sem, tok_s, tok_r, in_s, in_r,
    one_s, one_r, two_s, two_r, none_s, none_r, ntwo_s, ntwo_r,
    a0_s, a0_r, b0_s, b0_r, a1_s, a1_r, b1_s, b1_r, a2_s, a2_r, b2_s, b2_r,
    p2_s, p2_r, p3_s, p3_r, f_s, f_r,
):
    xh = lax.axis_index("task_0")
    Z = lax.axis_index("task_1")
    xl = lax.axis_index("dp_0")
    Y = lax.axis_index("dp_1")
    C = lax.axis_index("dp_2")
    X = xh * 2 + xl

    def dev(x, y, z, c):
        return (lax.div(x, 2), z, lax.rem(x, 2), y, c)

    def rem4(v):
        return lax.rem(v, 4)

    me = (X, Y, Z, C)
    xp, xm = dev(rem4(X + 1), Y, Z, C), dev(rem4(X + 3), Y, Z, C)
    yp, ym = dev(X, rem4(Y + 1), Z, C), dev(X, rem4(Y + 3), Z, C)
    zp, zm = dev(X, Y, rem4(Z + 1), C), dev(X, Y, rem4(Z + 3), C)
    partner = dev(X, Y, Z, 1 - C)

    def near(k):
        p = lax.rem(Y * 2 + C + k, 8)
        return dev(X, lax.div(p, 2), Z, lax.rem(p, 2))

    def far(k):
        p = lax.rem(X * 4 + Z + k, 16)
        return dev(lax.div(p, 4), Y, lax.rem(p, 4), C)

    def remote(src, dst, ssem, rsem, to):
        return pltpu.make_async_remote_copy(
            src_ref=src, dst_ref=dst, send_sem=ssem, recv_sem=rsem, device_id=to, device_id_type=MESH
        )

    def row0(x, z):
        return pl.multiple_of(lax.div(x, 2) * 2048 + z * 512 + lax.rem(x, 2) * 256, 256)

    def group(i):
        x = rem4(X + pick(i, DX))
        z = rem4(Z + pick(i, DZ))
        return x, z

    my_cols = pl.ds(pl.multiple_of(C * HALF, HALF), HALF)
    other_cols = pl.ds(pl.multiple_of((1 - C) * HALF, HALF), HALF)
    cp_idx = pltpu.make_async_copy(idx_hbm, idx.at[0], loc_sem.at[0])
    cp_cot = pltpu.make_async_copy(cot_hbm.at[:, my_cols], w.at[0], loc_sem.at[1])
    cp_idx.start()
    cp_cot.start()

    barrier = pltpu.get_barrier_semaphore()
    for k in range(1, 8):
        pl.semaphore_signal(barrier, inc=1, device_id=near(k), device_id_type=MESH)
    for k in range(1, 16):
        pl.semaphore_signal(barrier, inc=1, device_id=far(k), device_id_type=MESH)

    def local_tok(i):
        x, z = group(i)
        cols = pl.ds(row0(x, z), 256)
        return pltpu.make_async_copy(tok_hbm.at[:, cols], tok.at[0, :, cols], loc_sem.at[2 + i])

    def remote_tok(i):
        x, z = group(i)
        cols = pl.ds(row0(x, z), 256)
        return remote(tok_hbm.at[:, cols], tok.at[1, :, cols], tok_s.at[i], tok_r.at[i], partner)

    cp_idx.wait()
    own_idx = idx[0]
    here = Y * 2 + C
    for k in range(TASKS):
        cnt1[pl.ds(here, 1), pl.ds(k, 1), :] = jnp.sum(
            (own_idx == k).astype(jnp.int32), axis=0, keepdims=True
        )[None]
    pl.semaphore_wait(barrier, 22)

    def exchange(slots, at, count, to, ssem, rsem):
        copies = []
        for k in range(1, count):
            c = remote(slots.at[at], slots.at[at], ssem.at[k], rsem.at[k], to(k))
            c.start()
            copies.append(c)
        return copies

    def arrived(slots, at, count, to, ssem, rsem):
        for k in range(1, count):
            src = lax.rem(at + count - k, count)
            remote(slots.at[src], slots.at[src], ssem.at[k], rsem.at[k], to(k)).wait_recv()

    first = exchange(cnt1, here, 8, near, one_s, one_r)
    in_cot = remote(cot_hbm.at[:, other_cols], w.at[1], in_s.at[0], in_r.at[0], partner)
    in_idx = remote(idx_hbm, idx.at[1], in_s.at[1], in_r.at[1], partner)
    in_idx.start()
    in_cot.start()

    def start_tok(i, carry):
        local_tok(i).start()
        remote_tok(i).start()
        return carry

    lax.fori_loop(0, 16, start_tok, 0)

    arrived(cnt1, here, 8, near, one_s, one_r)
    plane = X * 4 + Z
    total = cnt1[0]
    for k in range(1, 8):
        total = total + cnt1[k]
    cnt2[plane] = total
    second = exchange(cnt2, plane, 16, far, two_s, two_r)
    arrived(cnt2, plane, 16, far, two_s, two_r)
    total = cnt2[0]
    for k in range(1, 16):
        total = total + cnt2[k]
    counts = jnp.sum(total, axis=1, keepdims=True)
    counts = jnp.broadcast_to(counts, (TASKS, 128)).astype(jnp.float32)

    in_idx.wait_recv()
    for s in range(2):
        ids = idx[s]
        scale = jnp.zeros((8, 128), jnp.float32)
        for k in range(TASKS):
            weight = lw_smem[k].astype(jnp.float32) / counts[k : k + 1, :]
            scale = jnp.where(ids == k, jnp.broadcast_to(weight, (8, 128)), scale)
        tsc[s] = scale
    cp_cot.wait()
    in_cot.wait_recv()

    for s in range(2):

        def weigh(b, carry):
            row = tsc[s, pl.ds(b, 1), :]
            mat = jnp.broadcast_to(row, (128, 128)).T
            rows = pl.ds(pl.multiple_of(b * 128, 128), 128)
            for j in range(HALF // 128):
                cols = pl.ds(j * 128, 128)
                w[s, rows, cols] = (w[s, rows, cols].astype(jnp.float32) * mat).astype(jnp.bfloat16)
            return carry

        lax.fori_loop(0, 8, weigh, 0)

    def A0(z, side):
        return remote(sA0.at[z, side], rA0.at[z, side], a0_s.at[z, side], a0_r.at[z, side], (xp, xm)[side])

    def B0(z, side):
        return remote(sB0.at[z, side], rB0.at[z, side], b0_s.at[z, side], b0_r.at[z, side], (xp, xm)[side])

    def A2(x, side):
        return remote(sA2.at[x, side], rA2.at[x, side], a2_s.at[x, side], a2_r.at[x, side], (zp, zm)[side])

    def B2(x, side):
        return remote(sB2.at[x, side], rB2.at[x, side], b2_s.at[x, side], b2_r.at[x, side], (zp, zm)[side])

    def A1(g, side):
        return remote(sA1.at[g, side], rA1.at[g, side], a1_s.at[g, side], a1_r.at[g, side], (yp, ym)[side])

    def B1(g, side):
        return remote(sB1.at[g, side], rB1.at[g, side], b1_s.at[g, side], b1_r.at[g, side], (yp, ym)[side])

    def first_phase(d, n, c0, width, own, A, B, sA, rA, sB):
        @pl.when(d == 2)
        def _():
            for side in range(2):
                encode(acc, 128 * side, 128, c0, width, sA.at[n, side])
                A(n, side).start()

        for side in range(2):

            @pl.when(d == 1 + 2 * side)
            def _():
                A(n, side).wait_recv()
                decode_add(acc, 128 * side, 128, c0, width, rA.at[n, side])
                encode(acc, 0, 256, c0, width, sB.at[n, side])
                B(n, side).start()

        @pl.when(d == 0)
        def _():
            copy_rows(own.at[n], 0, acc, 0, 256, c0, width)

    def late(i):
        x, z = group(i)
        g = x * 4 + z
        for side in range(2):
            A1(g, side).wait_recv()
            decode_add(hold1.at[g, side], 32 * side, 32, 0, W1, rA1.at[g, side])
            encode(hold1.at[g, side], 0, 64, 0, W1, sB1.at[g, side])
            B1(g, side).start()

    def step(i, carry):
        x, z = group(i)
        g = x * 4 + z
        cols = pl.ds(row0(x, z), 256)
        local_tok(i).wait()
        remote_tok(i).wait_recv()
        dims = (((0,), (0,)), ((), ()))
        acc[...] = lax.dot_general(
            tok[0, :, cols], w[0], dims, preferred_element_type=jnp.float32
        ) + lax.dot_general(tok[1, :, cols], w[1], dims, preferred_element_type=jnp.float32)
        dx = rem4(x + 4 - X)
        dz = rem4(z + 4 - Z)
        first_phase(dx, z, C0, W0, own0, A0, B0, sA0, rA0, sB0)
        y2 = pl.multiple_of(rem4(Y + 2) * 64, 64)
        for side in range(2):
            encode(acc, y2 + 32 * side, 32, C1, W1, sA1.at[g, side])
            A1(g, side).start()
        copy_rows(hold1.at[g, 0], 0, acc, pl.multiple_of(rem4(Y + 1) * 64, 64), 64, C1, W1)
        copy_rows(hold1.at[g, 1], 0, acc, pl.multiple_of(rem4(Y + 3) * 64, 64), 64, C1, W1)
        copy_rows(own1.at[z], pl.multiple_of(x * 64, 64), acc, pl.multiple_of(Y * 64, 64), 64, C1, W1)
        first_phase(dz, x, C2, W2, own2, A2, B2, sA2, rA2, sB2)

        @pl.when(i >= LAG)
        def _():
            late(i - LAG)

        return carry

    lax.fori_loop(0, 16, step, 0)

    def late_step(i, carry):
        late(i)
        return carry

    lax.fori_loop(16 - LAG, 16, late_step, 0)

    def ring(sA, rA, sB, rB, ss, rs, n, plus, minus):
        def A(side):
            return remote(sA.at[side], rA.at[side], ss.at[n, side], rs.at[n, side], (plus, minus)[side])

        def B(side):
            return remote(sB.at[side], rB.at[side], ss.at[n, 2 + side], rs.at[n, 2 + side], (plus, minus)[side])

        return A, B

    second_rings = (
        (own0, W0, Z, s2A.at[0], r2A.at[0], s2B.at[0], r2B.at[0], zp, zm),
        (own1, W1, Z, s2A.at[1], r2A.at[1], s2B.at[1], r2B.at[1], zp, zm),
        (own2, W2, X, s2A2, r2A2, s2B2, r2B2, xp, xm),
    )

    def gather(n, m):
        if n == 0:
            for side in range(2):
                B0(m, side).wait_recv()
                decode_add(own0.at[m], 0, 256, 0, W0, rB0.at[m, side])
        elif n == 2:
            for side in range(2):
                B2(m, side).wait_recv()
                decode_add(own2.at[m], 0, 256, 0, W2, rB2.at[m, side])
        else:

            def one(x, carry):
                g = x * 4 + m
                for side in range(2):
                    B1(g, side).wait_recv()
                    decode_add(own1.at[m], pl.multiple_of(x * 64, 64), 64, 0, W1, rB1.at[g, side])
                return carry

            lax.fori_loop(0, 4, one, 0)

    for n, (own, width, at, sA, rA, sB, rB, plus, minus) in enumerate(second_rings):
        A, B = ring(sA, rA, sB, rB, p2_s, p2_r, n, plus, minus)
        m = rem4(at + 2)
        gather(n, m)
        for side in range(2):
            encode(own.at[m], 128 * side, 128, 0, width, sA.at[side])
            A(side).start()
    for n, (own, width, at, sA, rA, sB, rB, plus, minus) in enumerate(second_rings):
        A, B = ring(sA, rA, sB, rB, p2_s, p2_r, n, plus, minus)
        for side in range(2):
            m = rem4(at + 1 + 2 * side)
            gather(n, m)
            A(side).wait_recv()
            decode_add(own.at[m], 128 * side, 128, 0, width, rA.at[side])
            encode(own.at[m], 0, 256, 0, width, sB.at[side])
            B(side).start()
    for n in range(3):
        gather(n, second_rings[n][2])
    for n, (own, width, at, sA, rA, sB, rB, plus, minus) in enumerate(second_rings):
        A, B = ring(sA, rA, sB, rB, p2_s, p2_r, n, plus, minus)
        for side in range(2):
            B(side).wait_recv()
            decode_add(own.at[at], 0, 256, 0, width, rB.at[side])

    third_rings = (
        (own0.at[Z], W0, Y, s3A.at[0], r3A.at[0], s3B.at[0], r3B.at[0], yp, ym),
        (own1.at[Z], W1, X, s3A.at[1], r3A.at[1], s3B.at[1], r3B.at[1], xp, xm),
        (own2.at[X], W2, Y, s3A2, r3A2, s3B2, r3B2, yp, ym),
    )
    for n, (own, width, at, sA, rA, sB, rB, plus, minus) in enumerate(third_rings):
        A, B = ring(sA, rA, sB, rB, p3_s, p3_r, n, plus, minus)
        r = pl.multiple_of(rem4(at + 2) * 64, 64)
        for side in range(2):
            encode(own, r + 32 * side, 32, 0, width, sA.at[side])
            A(side).start()
    for n, (own, width, at, sA, rA, sB, rB, plus, minus) in enumerate(third_rings):
        A, B = ring(sA, rA, sB, rB, p3_s, p3_r, n, plus, minus)
        for side in range(2):
            r = pl.multiple_of(rem4(at + 1 + 2 * side) * 64, 64)
            A(side).wait_recv()
            decode_add(own, r + 32 * side, 32, 0, width, rA.at[side])
            encode(own, r, 64, 0, width, sB.at[side])
            B(side).start()
    col = 0
    square = jnp.zeros((8, 128), jnp.float32)
    for n, (own, width, at, sA, rA, sB, rB, plus, minus) in enumerate(third_rings):
        A, B = ring(sA, rA, sB, rB, p3_s, p3_r, n, plus, minus)
        r = pl.multiple_of(at * 64, 64)
        for side in range(2):
            B(side).wait_recv()
            decode_add(own, r, 64, 0, width, rB.at[side])
        for t in range(8):
            for j in range(width // 128):
                v = own[pl.ds(r + t * 8, 8), pl.ds(j * 128, 128)]
                fin[pl.ds(t * 8, 8), pl.ds(col + j * 128, 128)] = v
                square = square + v * v
        col += width

    nrm1[here] = square
    third = exchange(nrm1, here, 8, near, none_s, none_r)
    theirs = pl.ds(pl.multiple_of((1 - C) * 32, 32), 32)
    mine = pl.ds(pl.multiple_of(C * 32, 32), 32)
    swap = remote(fin.at[theirs], finr, f_s, f_r, partner)
    swap.start()
    grad_ref[:, my_cols] = fin[mine, :]
    arrived(nrm1, here, 8, near, none_s, none_r)
    square = nrm1[0]
    for k in range(1, 8):
        square = square + nrm1[k]
    nrm2[plane] = square
    fourth = exchange(nrm2, plane, 16, far, ntwo_s, ntwo_r)
    swap.wait_recv()
    grad_ref[:, other_cols] = finr[...]

    def sent(z, carry):
        for side in range(2):
            A0(z, side).wait_send()
            B0(z, side).wait_send()
            A2(z, side).wait_send()
            B2(z, side).wait_send()
        return carry

    lax.fori_loop(0, 4, sent, 0)

    def sent1(g, carry):
        for side in range(2):
            A1(g, side).wait_send()
            B1(g, side).wait_send()
        remote_tok(g).wait_send()
        return carry

    lax.fori_loop(0, 16, sent1, 0)
    for rings, ss, rs in ((second_rings, p2_s, p2_r), (third_rings, p3_s, p3_r)):
        for n, (own, width, at, sA, rA, sB, rB, plus, minus) in enumerate(rings):
            A, B = ring(sA, rA, sB, rB, ss, rs, n, plus, minus)
            for side in range(2):
                A(side).wait_send()
                B(side).wait_send()
    in_cot.wait_send()
    in_idx.wait_send()
    swap.wait_send()
    for c in first + second + third + fourth:
        c.wait_send()

    arrived(nrm2, plane, 16, far, ntwo_s, ntwo_r)
    square = nrm2[0]
    for k in range(1, 16):
        square = square + nrm2[k]
    clip_ref[...] = jnp.broadcast_to(jnp.sum(square, keepdims=True), (8, 128))


def shards(tokens_in, query_cotangent, task_index, loss_weights, master, moment_first, moment_second):
    i16 = jnp.int16

    def msgs(lead, rows, width):
        return pltpu.VMEM((*lead, tiles(rows, width) + 1, 16, 128), i16)

    f32 = jnp.float32
    dma = pltpu.SemaphoreType.DMA
    scratch = [
        pltpu.VMEM((2, TOK, D), jnp.bfloat16),
        pltpu.VMEM((2, TOK, HALF), jnp.bfloat16),
        pltpu.VMEM((2, 8, 128), jnp.int32),
        pltpu.VMEM((2, 8, 128), f32),
        pltpu.VMEM((256, HALF), f32),
        pltpu.VMEM((4, 256, W0), f32),
        pltpu.VMEM((4, 256, W1), f32),
        pltpu.VMEM((4, 256, W2), f32),
        pltpu.VMEM((16, 2, 64, W1), f32),
        msgs((4, 2), 128, W0), msgs((4, 2), 128, W0), msgs((4, 2), 256, W0), msgs((4, 2), 256, W0),
        msgs((4, 2), 128, W2), msgs((4, 2), 128, W2), msgs((4, 2), 256, W2), msgs((4, 2), 256, W2),
        msgs((16, 2), 32, W1), msgs((16, 2), 32, W1), msgs((16, 2), 64, W1), msgs((16, 2), 64, W1),
        msgs((2, 2), 128, W0), msgs((2, 2), 128, W0), msgs((2, 2), 256, W0), msgs((2, 2), 256, W0),
        msgs((2,), 128, W2), msgs((2,), 128, W2), msgs((2,), 256, W2), msgs((2,), 256, W2),
        msgs((2, 2), 32, W0), msgs((2, 2), 32, W0), msgs((2, 2), 64, W0), msgs((2, 2), 64, W0),
        msgs((2,), 32, W2), msgs((2,), 32, W2), msgs((2,), 64, W2), msgs((2,), 64, W2),
        pltpu.VMEM((8, TASKS, 128), jnp.int32),
        pltpu.VMEM((16, TASKS, 128), jnp.int32),
        pltpu.VMEM((8, 8, 128), f32),
        pltpu.VMEM((16, 8, 128), f32),
        pltpu.VMEM((64, HALF), f32),
        pltpu.VMEM((32, HALF), f32),
        dma((18,)), dma((16,)), dma((16,)), dma((2,)), dma((2,)),
        dma((8,)), dma((8,)), dma((16,)), dma((16,)), dma((8,)), dma((8,)), dma((16,)), dma((16,)),
        dma((4, 2)), dma((4, 2)), dma((4, 2)), dma((4, 2)),
        dma((16, 2)), dma((16, 2)), dma((16, 2)), dma((16, 2)),
        dma((4, 2)), dma((4, 2)), dma((4, 2)), dma((4, 2)),
        dma((3, 4)), dma((3, 4)), dma((3, 4)), dma((3, 4)),
        dma(()), dma(()),
    ]
    hbm = pl.BlockSpec(memory_space=pl.ANY)
    vmem = pl.BlockSpec(memory_space=pltpu.VMEM)
    gradient, square = pl.pallas_call(
        kernel,
        out_shape=(
            jax.ShapeDtypeStruct((32, QW), f32),
            jax.ShapeDtypeStruct((8, 128), f32),
        ),
        in_specs=[hbm, hbm, hbm, pl.BlockSpec(memory_space=pltpu.SMEM)],
        out_specs=(vmem, vmem),
        scratch_shapes=scratch,
        compiler_params=pltpu.CompilerParams(
            collective_id=0, has_side_effects=True, vmem_limit_bytes=63 * 1024 * 1024
        ),
    )(tokens_in, query_cotangent, task_index.reshape(8, 128), loss_weights)
    root_mean = jnp.sqrt(square[0, 0] / (D * QW))
    factor = 1.0 / jnp.maximum(root_mean, 1.0)
    clipped = gradient * factor
    new_first = beta_one * moment_first + (1.0 - beta_one) * clipped
    new_second = beta_two * moment_second + (1.0 - beta_two) * clipped * clipped
    direction = new_first / corr_one / (jnp.sqrt(new_second / corr_two) + adam_eps)
    new_master = master - step_rate * (direction + decay_rate * master)
    return (new_master, new_first, new_second)


def solution(mesh):
    finer = Mesh(mesh.devices.reshape(2, 4, 2, 4, 2), AXES)
    rows = P(AXES, None)
    in_specs = (rows, rows, P(AXES), P(), rows, rows, rows)
    return jax.shard_map(
        shards, mesh=finer, in_specs=in_specs, out_specs=(rows, rows, rows), check_vma=False
    )
```

```python
import jax
import jax.numpy as jnp
from jax import lax
from jax.experimental import pallas as pl
from jax.experimental.pallas import tpu as pltpu
from jax.sharding import Mesh
from jax.sharding import PartitionSpec as P

D = 4096
QW = 2048
TASKS = 16
AXES = ("task_0", "task_1", "dp_0", "dp_1", "dp_2")
MESH = pl.DeviceIdType.MESH

beta_one = 0.9
beta_two = 0.95
adam_eps = 1e-08
step_rate = 0.01
decay_rate = 0.1
corr_one = 1.0 - 0.9**10
corr_two = 1.0 - 0.95**10

TOK = 1024
HALF = QW // 2
C0, W0 = 0, 384
C1, W1 = 384, 384
C2, W2 = 768, 256
LAG_B = 3
LAG_SUM = 6
SLOTS = 8
ORDER = (2, 1, 3, 0)
FETCH_X = (0, 1, 0, 2, 0, 3, 0, 1, 2, 1, 3, 1, 2, 3, 2, 3)
FETCH_Z = (0, 0, 1, 0, 2, 0, 3, 1, 1, 2, 1, 3, 2, 2, 3, 3)
NEED = (1, 2, 2, 2, 0, 1, 2, 2, 0, 0, 1, 2, 0, 0, 0, 1)
HAVE = (0, 1, 3, 5, 7, 7, 8, 10, 12, 12, 12, 13, 15, 15, 15, 15)
TOP = 32766.0


def pick(i, table):
    out = jnp.int32(table[0])
    for j in range(1, len(table)):
        out = jnp.where(i == j, jnp.int32(table[j]), out)
    return out


def tiles(rows, width):
    return (rows // 16) * (width // 128)


def encode(src, r0, rows, c0, width, msg):
    nc = width // 128
    unroll = min(8, rows // 16)

    def largest(t, ms):
        out = []
        for j in range(nc):
            a = jnp.abs(src[pl.ds(r0 + t * 16, 16), pl.ds(c0 + j * 128, 128)])
            out.append(jnp.maximum(ms[2 * j], a[:8]))
            out.append(jnp.maximum(ms[2 * j + 1], a[8:]))
        return tuple(out)

    zero = jnp.zeros((8, 128), jnp.float32)
    ms = lax.fori_loop(0, rows // 16, largest, (zero,) * (2 * nc), unroll=unroll)
    m = ms[0]
    for other in ms[1:]:
        m = jnp.maximum(m, other)
    e = jnp.ceil(jnp.log2(jnp.maximum(m, 1e-30)) + 0.001)
    inv = jnp.exp2(-e) * TOP
    inv = jnp.concatenate([inv, inv], axis=0)

    def put(t, carry):
        for j in range(nc):
            v = src[pl.ds(r0 + t * 16, 16), pl.ds(c0 + j * 128, 128)]
            msg[t * nc + j] = jnp.round(v * inv).astype(jnp.int32).astype(jnp.int16)
        return carry

    lax.fori_loop(0, rows // 16, put, 0, unroll=unroll)
    msg[tiles(rows, width)] = jnp.concatenate([e, e], axis=0).astype(jnp.int32).astype(jnp.int16)


def decode_sum(dst, dr0, dc0, src, sr0, sc0, rows, width, msgs):
    nc = width // 128
    scales = []
    for msg in msgs:
        e = msg[tiles(rows, width)].astype(jnp.int32).astype(jnp.float32)
        scales.append(jnp.exp2(e) * (1.0 / TOP))

    def add(t, carry):
        for j in range(nc):
            v = src[pl.ds(sr0 + t * 16, 16), pl.ds(sc0 + j * 128, 128)]
            for msg, scale in zip(msgs, scales):
                v = v + msg[t * nc + j].astype(jnp.int32).astype(jnp.float32) * scale
            dst[pl.ds(dr0 + t * 16, 16), pl.ds(dc0 + j * 128, 128)] = v
        return carry

    lax.fori_loop(0, rows // 16, add, 0, unroll=min(8, rows // 16))


def kernel(
    tok_hbm, cot_hbm, idx_hbm, lw_hbm, grad_ref,
    lw, tok, w, idx, tsc, acc,
    own0, own1, own2,
    sA0, rA0, sB0, rB0,
    sA2, rA2, sB2, rB2,
    sA1, rA1, sB1, rB1,
    s2A, r2A, s2B, r2B, s2A2, r2A2, s2B2, r2B2,
    s3, r3, s32, r32,
    cnt1, cnt2, nrm1, nrm2, fin, finr,
    loc_sem, tok_s, tok_r, in_s, in_r,
    one_s, one_r, two_s, two_r, none_s, none_r, ntwo_s, ntwo_r,
    a0_s, a0_r, b0_s, b0_r, a1_s, a1_r, b1_s, b1_r, a2_s, a2_r, b2_s, b2_r,
    p2a_s, p2a_r, p2b_s, p2b_r, p3_s, p3_r, f_s, f_r,
):
    xh = lax.axis_index("task_0")
    Z = lax.axis_index("task_1")
    xl = lax.axis_index("dp_0")
    Y = lax.axis_index("dp_1")
    C = lax.axis_index("dp_2")
    X = xh * 2 + xl

    def dev(x, y, z, c):
        return (lax.div(x, 2), z, lax.rem(x, 2), y, c)

    def rem4(v):
        return lax.rem(v, 4)

    me = (X, Y, Z, C)
    xp, xm = dev(rem4(X + 1), Y, Z, C), dev(rem4(X + 3), Y, Z, C)
    yp, ym = dev(X, rem4(Y + 1), Z, C), dev(X, rem4(Y + 3), Z, C)
    zp, zm = dev(X, Y, rem4(Z + 1), C), dev(X, Y, rem4(Z + 3), C)
    partner = dev(X, Y, Z, 1 - C)

    def near(k):
        p = lax.rem(Y * 2 + C + k, 8)
        return dev(X, lax.div(p, 2), Z, lax.rem(p, 2))

    def far(k):
        p = lax.rem(X * 4 + Z + k, 16)
        return dev(lax.div(p, 4), Y, lax.rem(p, 4), C)

    def remote(src, dst, ssem, rsem, to):
        return pltpu.make_async_remote_copy(
            src_ref=src, dst_ref=dst, send_sem=ssem, recv_sem=rsem, device_id=to, device_id_type=MESH
        )

    def row0(x, z):
        return pl.multiple_of(lax.div(x, 2) * 2048 + z * 512 + lax.rem(x, 2) * 256, 256)

    def place(p, q):
        return rem4(X + pick(p, ORDER)), rem4(Z + pick(q, ORDER))

    my_cols = pl.ds(pl.multiple_of(C * HALF, HALF), HALF)
    other_cols = pl.ds(pl.multiple_of((1 - C) * HALF, HALF), HALF)
    cp_idx = pltpu.make_async_copy(idx_hbm, idx.at[0], loc_sem.at[0])
    cp_cot = pltpu.make_async_copy(cot_hbm.at[:, my_cols], w.at[0], loc_sem.at[1])
    cp_lw = pltpu.make_async_copy(lw_hbm, lw, loc_sem.at[2])
    cp_idx.start()
    cp_lw.start()
    cp_cot.start()

    barrier = pltpu.get_barrier_semaphore()
    for k in range(1, 8):
        pl.semaphore_signal(barrier, inc=1, device_id=near(k), device_id_type=MESH)
    for k in range(1, 16):
        pl.semaphore_signal(barrier, inc=1, device_id=far(k), device_id_type=MESH)

    def local_tok(i):
        x, z = place(pick(i, FETCH_X), pick(i, FETCH_Z))
        cols = pl.ds(row0(x, z), 256)
        return pltpu.make_async_copy(tok_hbm.at[:, cols], tok.at[0, :, cols], loc_sem.at[3 + i])

    def remote_tok(i):
        x, z = place(pick(i, FETCH_X), pick(i, FETCH_Z))
        cols = pl.ds(row0(x, z), 256)
        return remote(tok_hbm.at[:, cols], tok.at[1, :, cols], tok_s, tok_r.at[i], partner)

    cp_idx.wait()
    own_idx = idx[0]
    here = Y * 2 + C
    lane = lax.broadcasted_iota(jnp.int32, (1, 128), 1)
    member = jnp.zeros((1, 128), jnp.int32)
    for k in range(TASKS):
        count = jnp.sum(jnp.sum((own_idx == k).astype(jnp.int32), axis=0, keepdims=True), axis=1, keepdims=True)
        member = jnp.where(lane == k, jnp.broadcast_to(count, (1, 128)), member)
    cnt1[here] = member
    pl.semaphore_wait(barrier, 22)

    def exchange(slots, at, count, to, ssem, rsem):
        for k in range(1, count):
            remote(slots.at[at], slots.at[at], ssem, rsem, to(k)).start()

    def everything(slots, count, ssem, rsem):
        some = slots.at[pl.ds(0, count - 1)]
        return remote(some, some, ssem, rsem, partner)

    def total_of(slots, count):
        total = slots[0]
        for k in range(1, count):
            total = total + slots[k]
        return total

    exchange(cnt1, here, 8, near, one_s, one_r)
    in_cot = remote(cot_hbm.at[:, other_cols], w.at[1], in_s.at[0], in_r.at[0], partner)
    in_idx = remote(idx_hbm, idx.at[1], in_s.at[1], in_r.at[1], partner)
    in_idx.start()
    in_cot.start()

    def start_tok(i, carry):
        local_tok(i).start()
        remote_tok(i).start()
        return carry

    lax.fori_loop(0, 16, start_tok, 0)

    everything(cnt1, 8, one_s, one_r).wait_recv()
    plane = X * 4 + Z
    cnt2[plane] = total_of(cnt1, 8)
    exchange(cnt2, plane, 16, far, two_s, two_r)
    everything(cnt2, 16, two_s, two_r).wait_recv()
    counts = jnp.broadcast_to(total_of(cnt2, 16), (TASKS, 128))
    diagonal = lax.broadcasted_iota(jnp.int32, (TASKS, 128), 0) == lax.broadcasted_iota(
        jnp.int32, (TASKS, 128), 1
    )
    counts = jnp.sum(jnp.where(diagonal, counts, 0), axis=1, keepdims=True)
    counts = jnp.broadcast_to(counts, (TASKS, 128)).astype(jnp.float32)
    cp_lw.wait()

    in_idx.wait_recv()
    for s in range(2):
        ids = idx[s]
        scale = jnp.zeros((8, 128), jnp.float32)
        for k in range(TASKS):
            weight = lw[k].astype(jnp.float32) / counts[k : k + 1, :]
            scale = jnp.where(ids == k, jnp.broadcast_to(weight, (8, 128)), scale)
        tsc[s] = scale
    cp_cot.wait()
    in_cot.wait_recv()

    for s in range(2):

        def weigh(b, carry):
            row = tsc[s, pl.ds(b, 1), :]
            mat = jnp.broadcast_to(row, (128, 128)).T
            rows = pl.ds(pl.multiple_of(b * 128, 128), 128)
            for j in range(HALF // 128):
                cols = pl.ds(j * 128, 128)
                w[s, rows, cols] = (w[s, rows, cols].astype(jnp.float32) * mat).astype(jnp.bfloat16)
            return carry

        lax.fori_loop(0, 8, weigh, 0)

    def message(S, R, ss, rs, ways):
        def at(n, side):
            return remote(S.at[n, side], R.at[n, side], ss, rs.at[n, side], ways[side])

        return at

    def halves(S, R, ss, rs, ways):
        def at(n, side, half):
            return remote(S.at[n, side, half], R.at[n, side, half], ss, rs.at[n], ways[side])

        return at

    def both(S, R, ss, rs, n):
        return remote(S.at[n], R.at[n], ss, rs.at[n], partner)

    A0 = message(sA0, rA0, a0_s, a0_r, (xp, xm))
    A1 = message(sA1, rA1, a1_s, a1_r, (yp, ym))
    A2 = message(sA2, rA2, a2_s, a2_r, (zp, zm))
    B0 = halves(sB0, rB0, b0_s, b0_r, (xp, xm))
    B1 = halves(sB1, rB1, b1_s, b1_r, (yp, ym))
    B2 = halves(sB2, rB2, b2_s, b2_r, (zp, zm))

    second_rings = (
        (own0, W0, s2A.at[0], r2A.at[0], s2B.at[0], r2B.at[0], zp, zm),
        (own1, W1, s2A.at[1], r2A.at[1], s2B.at[1], r2B.at[1], zp, zm),
        (own2, W2, s2A2, r2A2, s2B2, r2B2, xp, xm),
    )

    def A_second(n, side):
        own, width, sA, rA, sB, rB, plus, minus = second_rings[n]
        return remote(sA.at[side], rA.at[side], p2a_s.at[n], p2a_r.at[n, side], (plus, minus)[side])

    def B_second(n, side, half):
        own, width, sA, rA, sB, rB, plus, minus = second_rings[n]
        return remote(sB.at[side, half], rB.at[side, half], p2b_s.at[n], p2b_r.at[n], (plus, minus)[side])

    def second_phase(n, m, j):
        own, width, sA, rA, sB, rB, plus, minus = second_rings[n]
        chunk = own.at[m]

        @pl.when(j == 0)
        def _():
            for side in range(2):
                encode(chunk, 128 * side, 128, 0, width, sA.at[side])
            for side in range(2):
                A_second(n, side).start()

        for side in range(2):

            @pl.when(j == 1 + side)
            def _():
                encode(chunk, 128 * (1 - side), 128, 0, width, sB.at[side, 1 - side])
                B_second(n, side, 1 - side).start()
                A_second(n, side).wait_recv()
                r = 128 * side
                decode_sum(chunk, r, 0, chunk, r, 0, 128, width, [rA.at[side]])
                encode(chunk, r, 128, 0, width, sB.at[side, side])
                B_second(n, side, side).start()

    dims = (((0,), (0,)), ((), ()))

    def start_group(i):
        j, k = lax.div(i, 4), rem4(i)
        a = acc.at[lax.rem(i, SLOTS)]
        need, have = pick(i, NEED), pick(i, HAVE)
        for t in range(2):

            @pl.when(need > t)
            def _():
                local_tok(have + t).wait()
                remote_tok(have + t).wait_recv()

        x, z = place(k, j)
        x2, z2 = place(j, k)
        cols = pl.ds(row0(x, z), 256)
        cols2 = pl.ds(row0(x2, z2), 256)
        a[:, :C2] = lax.dot_general(
            tok[0, :, cols], w[0, :, :C2], dims, preferred_element_type=jnp.float32
        ) + lax.dot_general(tok[1, :, cols], w[1, :, :C2], dims, preferred_element_type=jnp.float32)
        a[:, C2:] = lax.dot_general(
            tok[0, :, cols2], w[0, :, C2:], dims, preferred_element_type=jnp.float32
        ) + lax.dot_general(tok[1, :, cols2], w[1, :, C2:], dims, preferred_element_type=jnp.float32)
        g = x * 4 + z
        y1, y2, y3 = (pl.multiple_of(rem4(Y + d) * 64, 64) for d in (1, 2, 3))
        encode(a, y2, 32, C1, W1, sA1.at[g, 0])
        encode(a, y2 + 32, 32, C1, W1, sA1.at[g, 1])
        encode(a, y1 + 32, 32, C1, W1, sB1.at[g, 0, 1])
        encode(a, y3, 32, C1, W1, sB1.at[g, 1, 0])
        for side in range(2):
            A1(g, side).start()
        for side in range(2):
            B1(g, side, 1 - side).start()

        @pl.when(k == 0)
        def _():
            for side in range(2):
                encode(a, 128 * side, 128, C0, W0, sA0.at[z, side])
                encode(a, 128 * side, 128, C2, W2, sA2.at[x2, side])
            for side in range(2):
                A0(z, side).start()
                A2(x2, side).start()

        for side in range(2):

            @pl.when(k == 1 + side)
            def _():
                r = 128 * (1 - side)
                encode(a, r, 128, C0, W0, sB0.at[z, side, 1 - side])
                encode(a, r, 128, C2, W2, sB2.at[x2, side, 1 - side])
                B0(z, side, 1 - side).start()
                B2(x2, side, 1 - side).start()

    def send_group(i):
        j, k = lax.div(i, 4), rem4(i)
        a = acc.at[lax.rem(i, SLOTS)]
        x, z = place(k, j)
        x2, z2 = place(j, k)
        g = x * 4 + z
        for side in range(2):
            A1(g, side).wait_recv()
        for side in range(2):
            r = pl.multiple_of(rem4(Y + 1 + 2 * side) * 64, 64) + 32 * side
            decode_sum(a, r, C1, a, r, C1, 32, W1, [rA1.at[g, side]])
            encode(a, r, 32, C1, W1, sB1.at[g, side, side])
        for side in range(2):
            B1(g, side, side).start()
        for side in range(2):

            @pl.when(k == 1 + side)
            def _():
                r = 128 * side
                A0(z, side).wait_recv()
                A2(x2, side).wait_recv()
                decode_sum(a, r, C0, a, r, C0, 128, W0, [rA0.at[z, side]])
                encode(a, r, 128, C0, W0, sB0.at[z, side, side])
                decode_sum(a, r, C2, a, r, C2, 128, W2, [rA2.at[x2, side]])
                encode(a, r, 128, C2, W2, sB2.at[x2, side, side])
                B0(z, side, side).start()
                B2(x2, side, side).start()

    def sum_group(i):
        j, k = lax.div(i, 4), rem4(i)
        a = acc.at[lax.rem(i, SLOTS)]
        x, z = place(k, j)
        x2, z2 = place(j, k)
        g = x * 4 + z
        both(sB1, rB1, b1_s, b1_r, g).wait_recv()
        mine = pl.multiple_of(Y * 64, 64)
        x64 = pl.multiple_of(x * 64, 64)
        for h in range(2):
            decode_sum(
                own1.at[z], x64 + 32 * h, 0, a, mine + 32 * h, C1, 32, W1, [rB1.at[g, 0, h], rB1.at[g, 1, h]]
            )

        @pl.when(k == 3)
        def _():
            both(sB0, rB0, b0_s, b0_r, z).wait_recv()
            for h in range(2):
                r = 128 * h
                decode_sum(own0.at[z], r, 0, a, r, C0, 128, W0, [rB0.at[z, 0, h], rB0.at[z, 1, h]])
            second_phase(0, z, j)
            second_phase(1, z, j)
            both(sB2, rB2, b2_s, b2_r, x2).wait_recv()
            for h in range(2):
                r = 128 * h
                decode_sum(own2.at[x2], r, 0, a, r, C2, 128, W2, [rB2.at[x2, 0, h], rB2.at[x2, 1, h]])
            second_phase(2, x2, j)

    def step(i, carry):
        @pl.when(i < 16)
        def _():
            start_group(i)

        @pl.when((i >= LAG_B) & (i < 16 + LAG_B))
        def _():
            send_group(i - LAG_B)

        @pl.when(i >= LAG_SUM)
        def _():
            sum_group(i - LAG_SUM)

        return carry

    lax.fori_loop(0, 16 + LAG_SUM, step, 0)

    def ring_y(d):
        return dev(X, rem4(Y + d), Z, C)

    def ring_x(d):
        return dev(rem4(X + d), Y, Z, C)

    third_rings = (
        (own0.at[Z], W0, Y, s3.at[0], r3.at[0], ring_y),
        (own1.at[Z], W1, X, s3.at[1], r3.at[1], ring_x),
        (own2.at[X], W2, Y, s32, r32, ring_y),
    )

    def third(n, d):
        own, width, at, S, R, to = third_rings[n]
        return remote(S.at[d - 1], R.at[d - 1], p3_s.at[n], p3_r.at[n], to(d))

    for n, m in ((0, Z), (1, Z), (2, X)):
        own, width, sA, rA, sB, rB, plus, minus = second_rings[n]
        remote(sB, rB, p2b_s.at[n], p2b_r.at[n], partner).wait_recv()
        for h in range(2):
            r = 128 * h
            decode_sum(own.at[m], r, 0, own.at[m], r, 0, 128, width, [rB.at[0, h], rB.at[1, h]])
        own, width, at, S, R, to = third_rings[n]
        for d in (2, 1, 3):
            encode(own, pl.multiple_of(rem4(at + d) * 64, 64), 64, 0, width, S.at[d - 1])
        for d in (2, 1, 3):
            third(n, d).start()
    col = 0
    square = jnp.zeros((8, 128), jnp.float32)
    for n, (own, width, at, S, R, to) in enumerate(third_rings):
        r = pl.multiple_of(at * 64, 64)
        remote(S, R, p3_s.at[n], p3_r.at[n], partner).wait_recv()
        decode_sum(own, r, 0, own, r, 0, 64, width, [R.at[d] for d in range(3)])
        for t in range(8):
            for j in range(width // 128):
                v = own[pl.ds(r + t * 8, 8), pl.ds(j * 128, 128)]
                fin[pl.ds(t * 8, 8), pl.ds(col + j * 128, 128)] = v
                square = square + v * v
        col += width

    nrm1[here] = jnp.sum(square, axis=0, keepdims=True)
    exchange(nrm1, here, 8, near, none_s, none_r)
    theirs = pl.ds(pl.multiple_of((1 - C) * 32, 32), 32)
    mine = pl.ds(pl.multiple_of(C * 32, 32), 32)
    swap = remote(fin.at[theirs], finr, f_s, f_r, partner)
    swap.start()
    everything(nrm1, 8, none_s, none_r).wait_recv()
    nrm2[plane] = total_of(nrm1, 8)
    exchange(nrm2, plane, 16, far, ntwo_s, ntwo_r)

    for S, ss in ((sA0, a0_s), (sB0, b0_s), (sA1, a1_s), (sB1, b1_s), (sA2, a2_s), (sB2, b2_s)):
        remote(S, S, ss, f_r, partner).wait_send()
    for n in range(3):
        own, width, sA, rA, sB, rB, plus, minus = second_rings[n]
        remote(sA, rA, p2a_s.at[n], f_r, partner).wait_send()
        remote(sB, rB, p2b_s.at[n], f_r, partner).wait_send()
        own, width, at, S, R, to = third_rings[n]
        remote(S, R, p3_s.at[n], f_r, partner).wait_send()
    remote(tok_hbm, tok.at[1], tok_s, f_r, partner).wait_send()
    in_cot.wait_send()
    in_idx.wait_send()
    for slots, count, ss in ((cnt1, 8, one_s), (cnt2, 16, two_s), (nrm1, 8, none_s), (nrm2, 16, ntwo_s)):
        everything(slots, count, ss, f_r).wait_send()
    swap.wait()
    everything(nrm2, 16, ntwo_s, ntwo_r).wait_recv()
    square = total_of(nrm2, 16)
    root_mean = jnp.sqrt(jnp.sum(square, keepdims=True) / (D * QW))
    factor = 1.0 / jnp.maximum(root_mean, 1.0)
    grad_ref[:, my_cols] = fin[mine, :] * factor
    grad_ref[:, other_cols] = finr[...] * factor


def shards(tokens_in, query_cotangent, task_index, loss_weights, master, moment_first, moment_second):
    i16 = jnp.int16

    def msgs(lead, rows, width):
        return pltpu.VMEM((*lead, tiles(rows, width) + 1, 16, 128), i16)

    f32 = jnp.float32
    dma = pltpu.SemaphoreType.DMA
    scratch = [
        pltpu.SMEM((TASKS,), jnp.int32),
        pltpu.VMEM((2, TOK, D), jnp.bfloat16),
        pltpu.VMEM((2, TOK, HALF), jnp.bfloat16),
        pltpu.VMEM((2, 8, 128), jnp.int32),
        pltpu.VMEM((2, 8, 128), f32),
        pltpu.VMEM((SLOTS, 256, HALF), f32),
        pltpu.VMEM((4, 256, W0), f32),
        pltpu.VMEM((4, 256, W1), f32),
        pltpu.VMEM((4, 256, W2), f32),
        msgs((4, 2), 128, W0), msgs((4, 2), 128, W0), msgs((4, 2, 2), 128, W0), msgs((4, 2, 2), 128, W0),
        msgs((4, 2), 128, W2), msgs((4, 2), 128, W2), msgs((4, 2, 2), 128, W2), msgs((4, 2, 2), 128, W2),
        msgs((16, 2), 32, W1), msgs((16, 2), 32, W1), msgs((16, 2, 2), 32, W1), msgs((16, 2, 2), 32, W1),
        msgs((2, 2), 128, W0), msgs((2, 2), 128, W0), msgs((2, 2, 2), 128, W0), msgs((2, 2, 2), 128, W0),
        msgs((2,), 128, W2), msgs((2,), 128, W2), msgs((2, 2), 128, W2), msgs((2, 2), 128, W2),
        msgs((2, 3), 64, W0), msgs((2, 3), 64, W0), msgs((3,), 64, W2), msgs((3,), 64, W2),
        pltpu.VMEM((8, 1, 128), jnp.int32),
        pltpu.VMEM((16, 1, 128), jnp.int32),
        pltpu.VMEM((8, 1, 128), f32),
        pltpu.VMEM((16, 1, 128), f32),
        pltpu.VMEM((64, HALF), f32),
        pltpu.VMEM((32, HALF), f32),
        dma((19,)), dma(()), dma((16,)), dma((2,)), dma((2,)),
        dma(()), dma(()), dma(()), dma(()), dma(()), dma(()), dma(()), dma(()),
        dma(()), dma((4, 2)), dma(()), dma((4,)),
        dma(()), dma((16, 2)), dma(()), dma((16,)),
        dma(()), dma((4, 2)), dma(()), dma((4,)),
        dma((3,)), dma((3, 2)), dma((3,)), dma((3,)), dma((3,)), dma((3,)),
        dma(()), dma(()),
    ]
    hbm = pl.BlockSpec(memory_space=pl.ANY)
    vmem = pl.BlockSpec(memory_space=pltpu.VMEM)
    clipped = pl.pallas_call(
        kernel,
        out_shape=jax.ShapeDtypeStruct((32, QW), f32),
        in_specs=[hbm] * 4,
        out_specs=vmem,
        scratch_shapes=scratch,
        compiler_params=pltpu.CompilerParams(
            collective_id=0, has_side_effects=True, vmem_limit_bytes=63 * 1024 * 1024
        ),
    )(tokens_in, query_cotangent, task_index.reshape(8, 128), loss_weights)
    new_first = beta_one * moment_first + (1.0 - beta_one) * clipped
    new_second = beta_two * moment_second + (1.0 - beta_two) * clipped * clipped
    direction = new_first / corr_one / (jnp.sqrt(new_second / corr_two) + adam_eps)
    new_master = master - step_rate * (direction + decay_rate * master)
    return (new_master, new_first, new_second)


def solution(mesh):
    finer = Mesh(mesh.devices.reshape(2, 4, 2, 4, 2), AXES)
    rows = P(AXES, None)
    in_specs = (rows, rows, P(AXES), P(), rows, rows, rows)
    return jax.shard_map(
        shards, mesh=finer, in_specs=in_specs, out_specs=(rows, rows, rows), check_vma=False
    )
```

```python
import jax
import jax.numpy as jnp
from jax import lax
from jax.experimental import pallas as pl
from jax.experimental.pallas import tpu as pltpu
from jax.sharding import Mesh
from jax.sharding import PartitionSpec as P

D = 4096
QW = 2048
TASKS = 16
AXES = ("task_0", "task_1", "dp_0", "dp_1", "dp_2")
MESH = pl.DeviceIdType.MESH

beta_one = 0.9
beta_two = 0.95
adam_eps = 1e-08
step_rate = 0.01
decay_rate = 0.1
corr_one = 1.0 - 0.9**10
corr_two = 1.0 - 0.95**10

TOK = 1024
HALF = QW // 2
C0, W0 = 0, 384
C1, W1 = 384, 384
C2, W2 = 768, 256
LAG_B = 3
LAG_SUM = 6
SLOTS = 8
ORDER = (2, 1, 3, 0)
FETCH_X = (0, 1, 0, 2, 0, 3, 0, 1, 2, 1, 3, 1, 2, 3, 2, 3)
FETCH_Z = (0, 0, 1, 0, 2, 0, 3, 1, 1, 2, 1, 3, 2, 2, 3, 3)
NEED = (1, 2, 2, 2, 0, 1, 2, 2, 0, 0, 1, 2, 0, 0, 0, 1)
HAVE = (0, 1, 3, 5, 7, 7, 8, 10, 12, 12, 12, 13, 15, 15, 15, 15)
TOP = 32766.0


def pick(i, table):
    out = jnp.int32(table[0])
    for j in range(1, len(table)):
        out = jnp.where(i == j, jnp.int32(table[j]), out)
    return out


def tiles(rows, width):
    return (rows // 16) * (width // 128)


def encode(src, starts, rows, c0, width, msg):
    nc = width // 128
    steps = rows // 16
    unroll = min(8, steps)
    ms = (jnp.zeros((8, 128), jnp.float32),) * (2 * nc)
    for r0 in starts:

        def largest(t, ms):
            out = []
            for j in range(nc):
                a = jnp.abs(src[pl.ds(r0 + t * 16, 16), pl.ds(c0 + j * 128, 128)])
                out.append(jnp.maximum(ms[2 * j], a[:8]))
                out.append(jnp.maximum(ms[2 * j + 1], a[8:]))
            return tuple(out)

        ms = lax.fori_loop(0, steps, largest, ms, unroll=unroll)
    m = ms[0]
    for other in ms[1:]:
        m = jnp.maximum(m, other)
    e = jnp.ceil(jnp.log2(jnp.maximum(m, 1e-30)) + 0.001)
    inv = jnp.exp2(-e) * TOP
    inv = jnp.concatenate([inv, inv], axis=0)
    for n, r0 in enumerate(starts):

        def put(t, carry):
            for j in range(nc):
                v = src[pl.ds(r0 + t * 16, 16), pl.ds(c0 + j * 128, 128)]
                msg[(n * steps + t) * nc + j] = jnp.round(v * inv).astype(jnp.int32).astype(jnp.int16)
            return carry

        lax.fori_loop(0, steps, put, 0, unroll=unroll)
    msg[msg.shape[0] - 1] = jnp.concatenate([e, e], axis=0).astype(jnp.int32).astype(jnp.int16)


def decode_sum(dst, dr0, dc0, src, sr0, sc0, rows, width, msgs):
    nc = width // 128
    scales = []
    for msg, _ in msgs:
        e = msg[msg.shape[0] - 1].astype(jnp.int32).astype(jnp.float32)
        scales.append(jnp.exp2(e) * (1.0 / TOP))

    def add(t, carry):
        for j in range(nc):
            v = src[pl.ds(sr0 + t * 16, 16), pl.ds(sc0 + j * 128, 128)]
            for (msg, first), scale in zip(msgs, scales):
                v = v + msg[first + t * nc + j].astype(jnp.int32).astype(jnp.float32) * scale
            dst[pl.ds(dr0 + t * 16, 16), pl.ds(dc0 + j * 128, 128)] = v
        return carry

    lax.fori_loop(0, rows // 16, add, 0, unroll=min(8, rows // 16))


def kernel(
    tok_hbm, cot_hbm, idx_hbm, lw_hbm, grad_ref,
    lw, tok, w, idx, tsc, acc,
    own0, own1, own2,
    sA0, rA0, sB0, rB0,
    sA2, rA2, sB2, rB2,
    sA1, rA1, sB1, rB1,
    s2A, r2A, s2B, r2B, s2A2, r2A2, s2B2, r2B2,
    s3, r3, s32, r32,
    cnt1, cnt2, nrm1, nrm2, fin, finr,
    loc_sem, tok_s, tok_r, in_s, in_r,
    one_s, one_r, two_s, two_r, none_s, none_r, ntwo_s, ntwo_r,
    a0_s, a0_r, b0_s, b0_r, a1_s, a1_r, b1_s, b1_r, a2_s, a2_r, b2_s, b2_r,
    p2a_s, p2a_r, p2b_s, p2b_r, p3_s, p3_r, f_s, f_r,
):
    xh = lax.axis_index("task_0")
    zz = lax.axis_index("task_1")
    xl = lax.axis_index("dp_0")
    Y = lax.axis_index("dp_1")
    C = lax.axis_index("dp_2")
    xx = xh * 2 + xl
    X = jnp.where(C == 0, xx, zz)
    Z = jnp.where(C == 0, zz, xx)

    def chip(x, y, z, c):
        return (lax.div(x, 2), z, lax.rem(x, 2), y, c)

    def dev(x, y, z, c):
        return chip(jnp.where(C == 0, x, z), y, jnp.where(C == 0, z, x), c)

    def rem4(v):
        return lax.rem(v, 4)

    me = (X, Y, Z, C)
    xp, xm = dev(rem4(X + 1), Y, Z, C), dev(rem4(X + 3), Y, Z, C)
    yp, ym = dev(X, rem4(Y + 1), Z, C), dev(X, rem4(Y + 3), Z, C)
    zp, zm = dev(X, Y, rem4(Z + 1), C), dev(X, Y, rem4(Z + 3), C)
    partner = chip(xx, Y, zz, 1 - C)

    def near(k):
        p = lax.rem(Y * 2 + C + k, 8)
        return chip(xx, lax.div(p, 2), zz, lax.rem(p, 2))

    def far(k):
        p = lax.rem(xx * 4 + zz + k, 16)
        return chip(lax.div(p, 4), Y, lax.rem(p, 4), C)

    def remote(src, dst, ssem, rsem, to):
        return pltpu.make_async_remote_copy(
            src_ref=src, dst_ref=dst, send_sem=ssem, recv_sem=rsem, device_id=to, device_id_type=MESH
        )

    def chip_row0(x, z):
        return pl.multiple_of(lax.div(x, 2) * 2048 + z * 512 + lax.rem(x, 2) * 256, 256)

    def row0(x, z):
        return chip_row0(jnp.where(C == 0, x, z), jnp.where(C == 0, z, x))

    def place(p, q):
        return rem4(X + pick(p, ORDER)), rem4(Z + pick(q, ORDER))

    my_cols = pl.ds(pl.multiple_of(C * HALF, HALF), HALF)
    other_cols = pl.ds(pl.multiple_of((1 - C) * HALF, HALF), HALF)
    cp_idx = pltpu.make_async_copy(idx_hbm, idx.at[0], loc_sem.at[0])
    cp_cot = pltpu.make_async_copy(cot_hbm.at[:, my_cols], w.at[0], loc_sem.at[1])
    cp_lw = pltpu.make_async_copy(lw_hbm, lw, loc_sem.at[2])
    cp_idx.start()
    cp_lw.start()
    cp_cot.start()

    barrier = pltpu.get_barrier_semaphore()
    for k in range(1, 8):
        pl.semaphore_signal(barrier, inc=1, device_id=near(k), device_id_type=MESH)
    for k in range(1, 16):
        pl.semaphore_signal(barrier, inc=1, device_id=far(k), device_id_type=MESH)

    def local_tok(i):
        x, z = place(pick(i, FETCH_X), pick(i, FETCH_Z))
        cols = pl.ds(row0(x, z), 256)
        return pltpu.make_async_copy(tok_hbm.at[:, cols], tok.at[0, :, cols], loc_sem.at[3 + i])

    def remote_tok(i):
        p, q = pick(i, FETCH_X), pick(i, FETCH_Z)
        p, q = jnp.where(C == 0, q, p), jnp.where(C == 0, p, q)
        cols = pl.ds(chip_row0(rem4(xx + pick(p, ORDER)), rem4(zz + pick(q, ORDER))), 256)
        return remote(tok_hbm.at[:, cols], tok.at[1, :, cols], tok_s, tok_r.at[i], partner)

    cp_idx.wait()
    own_idx = idx[0]
    here = Y * 2 + C
    lane = lax.broadcasted_iota(jnp.int32, (1, 128), 1)
    member = jnp.zeros((1, 128), jnp.int32)
    for k in range(TASKS):
        count = jnp.sum(jnp.sum((own_idx == k).astype(jnp.int32), axis=0, keepdims=True), axis=1, keepdims=True)
        member = jnp.where(lane == k, jnp.broadcast_to(count, (1, 128)), member)
    cnt1[here] = member
    pl.semaphore_wait(barrier, 22)

    def exchange(slots, at, count, to, ssem, rsem):
        for k in range(1, count):
            remote(slots.at[at], slots.at[at], ssem, rsem, to(k)).start()

    def everything(slots, count, ssem, rsem):
        some = slots.at[pl.ds(0, count - 1)]
        return remote(some, some, ssem, rsem, partner)

    def total_of(slots, count):
        total = slots[0]
        for k in range(1, count):
            total = total + slots[k]
        return total

    exchange(cnt1, here, 8, near, one_s, one_r)
    in_cot = remote(cot_hbm.at[:, other_cols], w.at[1], in_s.at[0], in_r.at[0], partner)
    in_idx = remote(idx_hbm, idx.at[1], in_s.at[1], in_r.at[1], partner)
    in_idx.start()
    in_cot.start()

    def start_tok(i, carry):
        local_tok(i).start()
        remote_tok(i).start()
        return carry

    lax.fori_loop(0, 5, start_tok, 0)

    everything(cnt1, 8, one_s, one_r).wait_recv()
    plane = xx * 4 + zz
    cnt2[plane] = total_of(cnt1, 8)
    exchange(cnt2, plane, 16, far, two_s, two_r)
    lax.fori_loop(5, 16, start_tok, 0)
    everything(cnt2, 16, two_s, two_r).wait_recv()
    counts = jnp.broadcast_to(total_of(cnt2, 16), (TASKS, 128))
    diagonal = lax.broadcasted_iota(jnp.int32, (TASKS, 128), 0) == lax.broadcasted_iota(
        jnp.int32, (TASKS, 128), 1
    )
    counts = jnp.sum(jnp.where(diagonal, counts, 0), axis=1, keepdims=True)
    counts = jnp.broadcast_to(counts, (TASKS, 128)).astype(jnp.float32)
    cp_lw.wait()

    in_idx.wait_recv()
    for s in range(2):
        ids = idx[s]
        scale = jnp.zeros((8, 128), jnp.float32)
        for k in range(TASKS):
            weight = lw[k].astype(jnp.float32) / counts[k : k + 1, :]
            scale = jnp.where(ids == k, jnp.broadcast_to(weight, (8, 128)), scale)
        tsc[s] = scale
    cp_cot.wait()
    in_cot.wait_recv()

    for s in range(2):

        def weigh(b, carry):
            row = tsc[s, pl.ds(b, 1), :]
            mat = jnp.broadcast_to(row, (128, 128)).T
            rows = pl.ds(pl.multiple_of(b * 128, 128), 128)
            for j in range(HALF // 128):
                cols = pl.ds(j * 128, 128)
                w[s, rows, cols] = (w[s, rows, cols].astype(jnp.float32) * mat).astype(jnp.bfloat16)
            return carry

        lax.fori_loop(0, 8, weigh, 0)

    def message(S, R, ss, rs, ways):
        def at(n, side):
            sem = rs.at[n, side] if len(rs.shape) == 2 else rs.at[n]
            return remote(S.at[n, side], R.at[n, side], ss, sem, ways[side])

        return at

    def halves(S, R, ss, rs, ways):
        def at(n, side, half):
            return remote(S.at[n, side, half], R.at[n, side, half], ss, rs.at[n], ways[side])

        return at

    def both(S, R, ss, rs, n):
        return remote(S.at[n], R.at[n], ss, rs.at[n], partner)

    A0 = message(sA0, rA0, a0_s, a0_r, (xp, xm))
    A1 = message(sA1, rA1, a1_s, a1_r, (yp, ym))
    B1 = message(sB1, rB1, b1_s, b1_r, (yp, ym))
    A2 = message(sA2, rA2, a2_s, a2_r, (zp, zm))
    B0 = halves(sB0, rB0, b0_s, b0_r, (xp, xm))
    B2 = halves(sB2, rB2, b2_s, b2_r, (zp, zm))

    second_rings = (
        (own0, W0, s2A.at[0], r2A.at[0], s2B.at[0], r2B.at[0], zp, zm),
        (own1, W1, s2A.at[1], r2A.at[1], s2B.at[1], r2B.at[1], zp, zm),
        (own2, W2, s2A2, r2A2, s2B2, r2B2, xp, xm),
    )

    def A_second(n, side):
        own, width, sA, rA, sB, rB, plus, minus = second_rings[n]
        return remote(sA.at[side], rA.at[side], p2a_s.at[n], p2a_r.at[n, side], (plus, minus)[side])

    def B_second(n, side, half):
        own, width, sA, rA, sB, rB, plus, minus = second_rings[n]
        return remote(sB.at[side, half], rB.at[side, half], p2b_s.at[n], p2b_r.at[n], (plus, minus)[side])

    def second_phase(n, m, j):
        own, width, sA, rA, sB, rB, plus, minus = second_rings[n]
        chunk = own.at[m]

        @pl.when(j == 0)
        def _():
            for side in range(2):
                encode(chunk, (128 * side,), 128, 0, width, sA.at[side])
            for side in range(2):
                A_second(n, side).start()

        for side in range(2):

            @pl.when(j == 1 + side)
            def _():
                encode(chunk, (128 * (1 - side),), 128, 0, width, sB.at[side, 1 - side])
                B_second(n, side, 1 - side).start()
                A_second(n, side).wait_recv()
                r = 128 * side
                decode_sum(chunk, r, 0, chunk, r, 0, 128, width, [(rA.at[side], 0)])
                encode(chunk, (r,), 128, 0, width, sB.at[side, side])
                B_second(n, side, side).start()

    dims = (((0,), (0,)), ((), ()))

    def start_group(i):
        j, k = lax.div(i, 4), rem4(i)
        a = acc.at[lax.rem(i, SLOTS)]
        need, have = pick(i, NEED), pick(i, HAVE)
        for t in range(2):

            @pl.when(need > t)
            def _():
                local_tok(have + t).wait()
                remote_tok(have + t).wait_recv()

        x, z = place(k, j)
        x2, z2 = place(j, k)
        cols = pl.ds(row0(x, z), 256)
        cols2 = pl.ds(row0(x2, z2), 256)
        a[:, :C2] = lax.dot_general(
            tok[0, :, cols], w[0, :, :C2], dims, preferred_element_type=jnp.float32
        ) + lax.dot_general(tok[1, :, cols], w[1, :, :C2], dims, preferred_element_type=jnp.float32)
        a[:, C2:] = lax.dot_general(
            tok[0, :, cols2], w[0, :, C2:], dims, preferred_element_type=jnp.float32
        ) + lax.dot_general(tok[1, :, cols2], w[1, :, C2:], dims, preferred_element_type=jnp.float32)
        g = x * 4 + z
        y1, y2, y3 = (pl.multiple_of(rem4(Y + d) * 64, 64) for d in (1, 2, 3))
        encode(a, (y2, y1 + 32), 32, C1, W1, sA1.at[g, 0])
        encode(a, (y2 + 32, y3), 32, C1, W1, sA1.at[g, 1])
        for side in range(2):
            A1(g, side).start()

        @pl.when(k == 0)
        def _():
            for side in range(2):
                encode(a, (128 * side,), 128, C0, W0, sA0.at[z, side])
                encode(a, (128 * side,), 128, C2, W2, sA2.at[x2, side])
            for side in range(2):
                A0(z, side).start()
                A2(x2, side).start()

        for side in range(2):

            @pl.when(k == 1 + side)
            def _():
                r = 128 * (1 - side)
                encode(a, (r,), 128, C0, W0, sB0.at[z, side, 1 - side])
                encode(a, (r,), 128, C2, W2, sB2.at[x2, side, 1 - side])
                B0(z, side, 1 - side).start()
                B2(x2, side, 1 - side).start()

    def send_group(i):
        j, k = lax.div(i, 4), rem4(i)
        a = acc.at[lax.rem(i, SLOTS)]
        x, z = place(k, j)
        x2, z2 = place(j, k)
        g = x * 4 + z
        for side in range(2):
            A1(g, side).wait_recv()
        for side in range(2):
            r = pl.multiple_of(rem4(Y + 1 + 2 * side) * 64, 64) + 32 * side
            decode_sum(a, r, C1, a, r, C1, 32, W1, [(rA1.at[g, side], 0)])
            encode(a, (r,), 32, C1, W1, sB1.at[g, side])
        for side in range(2):
            B1(g, side).start()
        for side in range(2):

            @pl.when(k == 1 + side)
            def _():
                r = 128 * side
                A0(z, side).wait_recv()
                A2(x2, side).wait_recv()
                decode_sum(a, r, C0, a, r, C0, 128, W0, [(rA0.at[z, side], 0)])
                encode(a, (r,), 128, C0, W0, sB0.at[z, side, side])
                decode_sum(a, r, C2, a, r, C2, 128, W2, [(rA2.at[x2, side], 0)])
                encode(a, (r,), 128, C2, W2, sB2.at[x2, side, side])
                B0(z, side, side).start()
                B2(x2, side, side).start()

    def sum_group(i):
        j, k = lax.div(i, 4), rem4(i)
        a = acc.at[lax.rem(i, SLOTS)]
        x, z = place(k, j)
        x2, z2 = place(j, k)
        g = x * 4 + z
        both(sB1, rB1, b1_s, b1_r, g).wait_recv()
        mine = pl.multiple_of(Y * 64, 64)
        x64 = pl.multiple_of(x * 64, 64)
        for h in range(2):
            parts = [(rB1.at[g, h], 0), (rA1.at[g, 1 - h], tiles(32, W1))]
            decode_sum(own1.at[z], x64 + 32 * h, 0, a, mine + 32 * h, C1, 32, W1, parts)

        @pl.when(k == 3)
        def _():
            both(sB0, rB0, b0_s, b0_r, z).wait_recv()
            for h in range(2):
                r = 128 * h
                decode_sum(own0.at[z], r, 0, a, r, C0, 128, W0, [(rB0.at[z, 0, h], 0), (rB0.at[z, 1, h], 0)])
            second_phase(0, z, j)
            second_phase(1, z, j)
            both(sB2, rB2, b2_s, b2_r, x2).wait_recv()
            for h in range(2):
                r = 128 * h
                decode_sum(own2.at[x2], r, 0, a, r, C2, 128, W2, [(rB2.at[x2, 0, h], 0), (rB2.at[x2, 1, h], 0)])
            second_phase(2, x2, j)

    def step(i, carry):
        @pl.when(i < 16)
        def _():
            start_group(i)

        @pl.when((i >= LAG_B) & (i < 16 + LAG_B))
        def _():
            send_group(i - LAG_B)

        @pl.when(i >= LAG_SUM)
        def _():
            sum_group(i - LAG_SUM)

        return carry

    lax.fori_loop(0, 16 + LAG_SUM, step, 0)

    def ring_y(d):
        return dev(X, rem4(Y + d), Z, C)

    def ring_x(d):
        return dev(rem4(X + d), Y, Z, C)

    third_rings = (
        (own0.at[Z], W0, Y, s3.at[0], r3.at[0], ring_y),
        (own1.at[Z], W1, X, s3.at[1], r3.at[1], ring_x),
        (own2.at[X], W2, Y, s32, r32, ring_y),
    )

    def third(n, d):
        own, width, at, S, R, to = third_rings[n]
        return remote(S.at[d - 1], R.at[d - 1], p3_s.at[n], p3_r.at[n], to(d))

    for n, m in ((0, Z), (1, Z), (2, X)):
        own, width, sA, rA, sB, rB, plus, minus = second_rings[n]
        remote(sB, rB, p2b_s.at[n], p2b_r.at[n], partner).wait_recv()
        for h in range(2):
            r = 128 * h
            decode_sum(own.at[m], r, 0, own.at[m], r, 0, 128, width, [(rB.at[0, h], 0), (rB.at[1, h], 0)])
        own, width, at, S, R, to = third_rings[n]
        for d in (2, 1, 3):
            encode(own, (pl.multiple_of(rem4(at + d) * 64, 64),), 64, 0, width, S.at[d - 1])
        for d in (2, 1, 3):
            third(n, d).start()
    col = 0
    square = jnp.zeros((8, 128), jnp.float32)
    for n, (own, width, at, S, R, to) in enumerate(third_rings):
        r = pl.multiple_of(at * 64, 64)
        remote(S, R, p3_s.at[n], p3_r.at[n], partner).wait_recv()
        decode_sum(own, r, 0, own, r, 0, 64, width, [(R.at[d], 0) for d in range(3)])
        for t in range(8):
            for j in range(width // 128):
                v = own[pl.ds(r + t * 8, 8), pl.ds(j * 128, 128)]
                fin[pl.ds(t * 8, 8), pl.ds(col + j * 128, 128)] = v
                square = square + v * v
        col += width

    nrm1[here] = jnp.sum(square, axis=0, keepdims=True)
    exchange(nrm1, here, 8, near, none_s, none_r)
    theirs = pl.ds(pl.multiple_of((1 - C) * 32, 32), 32)
    mine = pl.ds(pl.multiple_of(C * 32, 32), 32)
    swap = remote(fin.at[theirs], finr, f_s, f_r, partner)
    swap.start()
    everything(nrm1, 8, none_s, none_r).wait_recv()
    nrm2[plane] = total_of(nrm1, 8)
    exchange(nrm2, plane, 16, far, ntwo_s, ntwo_r)

    for S, ss in ((sA0, a0_s), (sB0, b0_s), (sA1, a1_s), (sB1, b1_s), (sA2, a2_s), (sB2, b2_s)):
        remote(S, S, ss, f_r, partner).wait_send()
    for n in range(3):
        own, width, sA, rA, sB, rB, plus, minus = second_rings[n]
        remote(sA, rA, p2a_s.at[n], f_r, partner).wait_send()
        remote(sB, rB, p2b_s.at[n], f_r, partner).wait_send()
        own, width, at, S, R, to = third_rings[n]
        remote(S, R, p3_s.at[n], f_r, partner).wait_send()
    remote(tok_hbm, tok.at[1], tok_s, f_r, partner).wait_send()
    in_cot.wait_send()
    in_idx.wait_send()
    for slots, count, ss in ((cnt1, 8, one_s), (cnt2, 16, two_s), (nrm1, 8, none_s), (nrm2, 16, ntwo_s)):
        everything(slots, count, ss, f_r).wait_send()
    swap.wait()
    everything(nrm2, 16, ntwo_s, ntwo_r).wait_recv()
    square = total_of(nrm2, 16)
    root_mean = jnp.sqrt(jnp.sum(square, keepdims=True) / (D * QW))
    factor = 1.0 / jnp.maximum(root_mean, 1.0)
    grad_ref[:, my_cols] = fin[mine, :] * factor
    grad_ref[:, other_cols] = finr[...] * factor


def shards(tokens_in, query_cotangent, task_index, loss_weights, master, moment_first, moment_second):
    i16 = jnp.int16

    def msgs(lead, rows, width):
        return pltpu.VMEM((*lead, tiles(rows, width) + 1, 16, 128), i16)

    f32 = jnp.float32
    dma = pltpu.SemaphoreType.DMA
    scratch = [
        pltpu.SMEM((TASKS,), jnp.int32),
        pltpu.VMEM((2, TOK, D), jnp.bfloat16),
        pltpu.VMEM((2, TOK, HALF), jnp.bfloat16),
        pltpu.VMEM((2, 8, 128), jnp.int32),
        pltpu.VMEM((2, 8, 128), f32),
        pltpu.VMEM((SLOTS, 256, HALF), f32),
        pltpu.VMEM((4, 256, W0), f32),
        pltpu.VMEM((4, 256, W1), f32),
        pltpu.VMEM((4, 256, W2), f32),
        msgs((4, 2), 128, W0), msgs((4, 2), 128, W0), msgs((4, 2, 2), 128, W0), msgs((4, 2, 2), 128, W0),
        msgs((4, 2), 128, W2), msgs((4, 2), 128, W2), msgs((4, 2, 2), 128, W2), msgs((4, 2, 2), 128, W2),
        msgs((16, 2), 64, W1), msgs((16, 2), 64, W1), msgs((16, 2), 32, W1), msgs((16, 2), 32, W1),
        msgs((2, 2), 128, W0), msgs((2, 2), 128, W0), msgs((2, 2, 2), 128, W0), msgs((2, 2, 2), 128, W0),
        msgs((2,), 128, W2), msgs((2,), 128, W2), msgs((2, 2), 128, W2), msgs((2, 2), 128, W2),
        msgs((2, 3), 64, W0), msgs((2, 3), 64, W0), msgs((3,), 64, W2), msgs((3,), 64, W2),
        pltpu.VMEM((8, 1, 128), jnp.int32),
        pltpu.VMEM((16, 1, 128), jnp.int32),
        pltpu.VMEM((8, 1, 128), f32),
        pltpu.VMEM((16, 1, 128), f32),
        pltpu.VMEM((64, HALF), f32),
        pltpu.VMEM((32, HALF), f32),
        dma((19,)), dma(()), dma((16,)), dma((2,)), dma((2,)),
        dma(()), dma(()), dma(()), dma(()), dma(()), dma(()), dma(()), dma(()),
        dma(()), dma((4, 2)), dma(()), dma((4,)),
        dma(()), dma((16, 2)), dma(()), dma((16,)),
        dma(()), dma((4, 2)), dma(()), dma((4,)),
        dma((3,)), dma((3, 2)), dma((3,)), dma((3,)), dma((3,)), dma((3,)),
        dma(()), dma(()),
    ]
    hbm = pl.BlockSpec(memory_space=pl.ANY)
    vmem = pl.BlockSpec(memory_space=pltpu.VMEM)
    clipped = pl.pallas_call(
        kernel,
        out_shape=jax.ShapeDtypeStruct((32, QW), f32),
        in_specs=[hbm] * 4,
        out_specs=vmem,
        scratch_shapes=scratch,
        compiler_params=pltpu.CompilerParams(
            collective_id=0, has_side_effects=True, vmem_limit_bytes=63 * 1024 * 1024
        ),
    )(tokens_in, query_cotangent, task_index.reshape(8, 128), loss_weights)
    new_first = beta_one * moment_first + (1.0 - beta_one) * clipped
    new_second = beta_two * moment_second + (1.0 - beta_two) * clipped * clipped
    direction = new_first / corr_one / (jnp.sqrt(new_second / corr_two) + adam_eps)
    new_master = master - step_rate * (direction + decay_rate * master)
    return (new_master, new_first, new_second)


def solution(mesh):
    finer = Mesh(mesh.devices.reshape(2, 4, 2, 4, 2), AXES)
    rows = P(AXES, None)
    in_specs = (rows, rows, P(AXES), P(), rows, rows, rows)
    return jax.shard_map(
        shards, mesh=finer, in_specs=in_specs, out_specs=(rows, rows, rows), check_vma=False
    )
```

```python
import jax
import jax.numpy as jnp
from jax import lax
from jax.experimental import pallas as pl
from jax.experimental.pallas import tpu as pltpu
from jax.sharding import Mesh
from jax.sharding import PartitionSpec as P

D = 4096
QW = 2048
TASKS = 16
AXES = ("task_0", "task_1", "dp_0", "dp_1", "dp_2")
MESH = pl.DeviceIdType.MESH

beta_one = 0.9
beta_two = 0.95
adam_eps = 1e-08
step_rate = 0.01
decay_rate = 0.1
corr_one = 1.0 - 0.9**10
corr_two = 1.0 - 0.95**10

TOK = 1024
HALF = QW // 2
C0, W0 = 0, 384
C1, W1 = 384, 384
C2, W2 = 768, 256
LAG_B = 3
LAG_SUM = 6
SLOTS = 8
ORDER = (2, 1, 3, 0)
FETCH_X = (0, 1, 0, 2, 0, 3, 0, 1, 2, 1, 3, 1, 2, 3, 2, 3)
FETCH_Z = (0, 0, 1, 0, 2, 0, 3, 1, 1, 2, 1, 3, 2, 2, 3, 3)
NEED = (1, 2, 2, 2, 0, 1, 2, 2, 0, 0, 1, 2, 0, 0, 0, 1)
HAVE = (0, 1, 3, 5, 7, 7, 8, 10, 12, 12, 12, 13, 15, 15, 15, 15)
TOP = 32766.0


def pick(i, table):
    out = jnp.int32(table[0])
    for j in range(1, len(table)):
        out = jnp.where(i == j, jnp.int32(table[j]), out)
    return out


def tiles(rows, width):
    return (rows // 16) * (width // 128)


def encode(src, starts, rows, c0, width, msg):
    nc = width // 128
    steps = rows // 16
    unroll = min(8, steps)
    ms = (jnp.zeros((8, 128), jnp.float32),) * (2 * nc)
    for r0 in starts:

        def largest(t, ms):
            out = []
            for j in range(nc):
                a = jnp.abs(src[pl.ds(r0 + t * 16, 16), pl.ds(c0 + j * 128, 128)])
                out.append(jnp.maximum(ms[2 * j], a[:8]))
                out.append(jnp.maximum(ms[2 * j + 1], a[8:]))
            return tuple(out)

        ms = lax.fori_loop(0, steps, largest, ms, unroll=unroll)
    m = ms[0]
    for other in ms[1:]:
        m = jnp.maximum(m, other)
    e = jnp.ceil(jnp.log2(jnp.maximum(m, 1e-30)) + 0.001)
    inv = jnp.exp2(-e) * TOP
    inv = jnp.concatenate([inv, inv], axis=0)
    for n, r0 in enumerate(starts):

        def put(t, carry):
            for j in range(nc):
                v = src[pl.ds(r0 + t * 16, 16), pl.ds(c0 + j * 128, 128)]
                msg[(n * steps + t) * nc + j] = jnp.round(v * inv).astype(jnp.int32).astype(jnp.int16)
            return carry

        lax.fori_loop(0, steps, put, 0, unroll=unroll)
    msg[msg.shape[0] - 1] = jnp.concatenate([e, e], axis=0).astype(jnp.int32).astype(jnp.int16)


def decode_sum(dst, dr0, dc0, src, sr0, sc0, rows, width, msgs):
    nc = width // 128
    scales = []
    for msg, _ in msgs:
        e = msg[msg.shape[0] - 1].astype(jnp.int32).astype(jnp.float32)
        scales.append(jnp.exp2(e) * (1.0 / TOP))

    def add(t, carry):
        for j in range(nc):
            v = src[pl.ds(sr0 + t * 16, 16), pl.ds(sc0 + j * 128, 128)]
            for (msg, first), scale in zip(msgs, scales):
                v = v + msg[first + t * nc + j].astype(jnp.int32).astype(jnp.float32) * scale
            dst[pl.ds(dr0 + t * 16, 16), pl.ds(dc0 + j * 128, 128)] = v
        return carry

    lax.fori_loop(0, rows // 16, add, 0, unroll=min(8, rows // 16))


def kernel(
    tok_hbm, cot_hbm, idx_hbm, lw_hbm, grad_ref,
    lw, tok, w, idx, tsc, acc,
    own0, own1, own2,
    sA0, rA0, sB0, rB0,
    sA2, rA2, sB2, rB2,
    sA1, rA1, sB1, rB1,
    s2A, r2A, s2B, r2B, s2A2, r2A2, s2B2, r2B2,
    s3, r3, s32, r32,
    cnt1, cnt2, nrm1, nrm2, fin, finr,
    loc_sem, tok_s, tok_r, in_s, in_r,
    one_s, one_r, two_s, two_r, none_s, none_r, ntwo_s, ntwo_r,
    a0_s, a0_r, b0_s, b0_r, a1_s, a1_r, b1_s, b1_r, a2_s, a2_r, b2_s, b2_r,
    p2a_s, p2a_r, p2b_s, p2b_r, p3_s, p3_r, f_s, f_r,
):
    xh = lax.axis_index("task_0")
    zz = lax.axis_index("task_1")
    xl = lax.axis_index("dp_0")
    Y = lax.axis_index("dp_1")
    C = lax.axis_index("dp_2")
    xx = xh * 2 + xl
    X = jnp.where(C == 0, xx, zz)
    Z = jnp.where(C == 0, zz, xx)

    def chip(x, y, z, c):
        return (lax.div(x, 2), z, lax.rem(x, 2), y, c)

    def dev(x, y, z, c):
        return chip(jnp.where(C == 0, x, z), y, jnp.where(C == 0, z, x), c)

    def rem4(v):
        return lax.rem(v, 4)

    me = (X, Y, Z, C)
    xp, xm = dev(rem4(X + 1), Y, Z, C), dev(rem4(X + 3), Y, Z, C)
    yp, ym = dev(X, rem4(Y + 1), Z, C), dev(X, rem4(Y + 3), Z, C)
    zp, zm = dev(X, Y, rem4(Z + 1), C), dev(X, Y, rem4(Z + 3), C)
    partner = chip(xx, Y, zz, 1 - C)

    def near(k):
        p = lax.rem(Y * 2 + C + k, 8)
        return chip(xx, lax.div(p, 2), zz, lax.rem(p, 2))

    def far(k):
        p = lax.rem(xx * 4 + zz + k, 16)
        return chip(lax.div(p, 4), Y, lax.rem(p, 4), C)

    def remote(src, dst, ssem, rsem, to):
        return pltpu.make_async_remote_copy(
            src_ref=src, dst_ref=dst, send_sem=ssem, recv_sem=rsem, device_id=to, device_id_type=MESH
        )

    def chip_row0(x, z):
        return pl.multiple_of(lax.div(x, 2) * 2048 + z * 512 + lax.rem(x, 2) * 256, 256)

    def row0(x, z):
        return chip_row0(jnp.where(C == 0, x, z), jnp.where(C == 0, z, x))

    def place(p, q):
        return rem4(X + pick(p, ORDER)), rem4(Z + pick(q, ORDER))

    my_cols = pl.ds(pl.multiple_of(C * HALF, HALF), HALF)
    other_cols = pl.ds(pl.multiple_of((1 - C) * HALF, HALF), HALF)
    cp_idx = pltpu.make_async_copy(idx_hbm, idx.at[0], loc_sem.at[0])
    cp_cot = pltpu.make_async_copy(cot_hbm.at[:, my_cols], w.at[0], loc_sem.at[1])
    cp_lw = pltpu.make_async_copy(lw_hbm, lw, loc_sem.at[2])
    cp_idx.start()
    cp_lw.start()
    cp_cot.start()

    barrier = pltpu.get_barrier_semaphore()
    for k in range(1, 8):
        pl.semaphore_signal(barrier, inc=1, device_id=near(k), device_id_type=MESH)
    for k in range(1, 16):
        pl.semaphore_signal(barrier, inc=1, device_id=far(k), device_id_type=MESH)

    def local_tok(i):
        x, z = place(pick(i, FETCH_X), pick(i, FETCH_Z))
        cols = pl.ds(row0(x, z), 256)
        return pltpu.make_async_copy(tok_hbm.at[:, cols], tok.at[0, :, cols], loc_sem.at[3 + i])

    def remote_tok(i):
        p, q = pick(i, FETCH_X), pick(i, FETCH_Z)
        p, q = jnp.where(C == 0, q, p), jnp.where(C == 0, p, q)
        cols = pl.ds(chip_row0(rem4(xx + pick(p, ORDER)), rem4(zz + pick(q, ORDER))), 256)
        return remote(tok_hbm.at[:, cols], tok.at[1, :, cols], tok_s, tok_r.at[i], partner)

    cp_idx.wait()
    own_idx = idx[0]
    here = Y * 2 + C
    lane = lax.broadcasted_iota(jnp.int32, (1, 128), 1)
    member = jnp.zeros((1, 128), jnp.int32)
    for k in range(TASKS):
        count = jnp.sum(jnp.sum((own_idx == k).astype(jnp.int32), axis=0, keepdims=True), axis=1, keepdims=True)
        member = jnp.where(lane == k, jnp.broadcast_to(count, (1, 128)), member)
    cnt1[here] = member
    pl.semaphore_wait(barrier, 22)

    def exchange(slots, at, count, to, ssem, rsem):
        for k in range(1, count):
            remote(slots.at[at], slots.at[at], ssem, rsem, to(k)).start()

    def everything(slots, count, ssem, rsem):
        some = slots.at[pl.ds(0, count - 1)]
        return remote(some, some, ssem, rsem, partner)

    def total_of(slots, count):
        total = slots[0]
        for k in range(1, count):
            total = total + slots[k]
        return total

    exchange(cnt1, here, 8, near, one_s, one_r)
    in_cot = remote(cot_hbm.at[:, other_cols], w.at[1], in_s.at[0], in_r.at[0], partner)
    in_idx = remote(idx_hbm, idx.at[1], in_s.at[1], in_r.at[1], partner)
    in_idx.start()
    in_cot.start()

    def start_tok(i, carry):
        local_tok(i).start()
        remote_tok(i).start()
        return carry

    lax.fori_loop(0, 5, start_tok, 0)

    everything(cnt1, 8, one_s, one_r).wait_recv()
    plane = xx * 4 + zz
    cnt2[plane] = total_of(cnt1, 8)
    exchange(cnt2, plane, 16, far, two_s, two_r)
    lax.fori_loop(5, 16, start_tok, 0)
    everything(cnt2, 16, two_s, two_r).wait_recv()
    counts = jnp.broadcast_to(total_of(cnt2, 16), (TASKS, 128))
    diagonal = lax.broadcasted_iota(jnp.int32, (TASKS, 128), 0) == lax.broadcasted_iota(
        jnp.int32, (TASKS, 128), 1
    )
    counts = jnp.sum(jnp.where(diagonal, counts, 0), axis=1, keepdims=True)
    counts = jnp.broadcast_to(counts, (TASKS, 128)).astype(jnp.float32)
    cp_lw.wait()

    in_idx.wait_recv()
    for s in range(2):
        ids = idx[s]
        scale = jnp.zeros((8, 128), jnp.float32)
        for k in range(TASKS):
            weight = lw[k].astype(jnp.float32) / counts[k : k + 1, :]
            scale = jnp.where(ids == k, jnp.broadcast_to(weight, (8, 128)), scale)
        tsc[s] = scale
    cp_cot.wait()
    in_cot.wait_recv()

    for s in range(2):

        def weigh(b, carry):
            row = tsc[s, pl.ds(b, 1), :]
            mat = jnp.broadcast_to(row, (128, 128)).T
            rows = pl.ds(pl.multiple_of(b * 128, 128), 128)
            for j in range(HALF // 128):
                cols = pl.ds(j * 128, 128)
                w[s, rows, cols] = (w[s, rows, cols].astype(jnp.float32) * mat).astype(jnp.bfloat16)
            return carry

        lax.fori_loop(0, 8, weigh, 0, unroll=4)

    def message(S, R, ss, rs, ways):
        def at(n, side):
            sem = rs.at[n, side] if len(rs.shape) == 2 else rs.at[n]
            return remote(S.at[n, side], R.at[n, side], ss, sem, ways[side])

        return at

    def halves(S, R, ss, rs, ways):
        def at(n, side, half):
            return remote(S.at[n, side, half], R.at[n, side, half], ss, rs.at[n], ways[side])

        return at

    def both(S, R, ss, rs, n):
        return remote(S.at[n], R.at[n], ss, rs.at[n], partner)

    A0 = message(sA0, rA0, a0_s, a0_r, (xp, xm))
    A1 = message(sA1, rA1, a1_s, a1_r, (yp, ym))
    B1 = message(sB1, rB1, b1_s, b1_r, (yp, ym))
    A2 = message(sA2, rA2, a2_s, a2_r, (zp, zm))
    B0 = halves(sB0, rB0, b0_s, b0_r, (xp, xm))
    B2 = halves(sB2, rB2, b2_s, b2_r, (zp, zm))

    second_rings = (
        (own0, W0, s2A.at[0], r2A.at[0], s2B.at[0], r2B.at[0], zp, zm),
        (own1, W1, s2A.at[1], r2A.at[1], s2B.at[1], r2B.at[1], zp, zm),
        (own2, W2, s2A2, r2A2, s2B2, r2B2, xp, xm),
    )

    def A_second(n, side):
        own, width, sA, rA, sB, rB, plus, minus = second_rings[n]
        return remote(sA.at[side], rA.at[side], p2a_s.at[n], p2a_r.at[n, side], (plus, minus)[side])

    def B_second(n, side, half):
        own, width, sA, rA, sB, rB, plus, minus = second_rings[n]
        return remote(sB.at[side, half], rB.at[side, half], p2b_s.at[n], p2b_r.at[n], (plus, minus)[side])

    def second_phase(n, m, j):
        own, width, sA, rA, sB, rB, plus, minus = second_rings[n]
        chunk = own.at[m]

        @pl.when(j == 0)
        def _():
            for side in range(2):
                encode(chunk, (128 * side,), 128, 0, width, sA.at[side])
            for side in range(2):
                A_second(n, side).start()

        for side in range(2):

            @pl.when(j == 1 + side)
            def _():
                encode(chunk, (128 * (1 - side),), 128, 0, width, sB.at[side, 1 - side])
                B_second(n, side, 1 - side).start()
                A_second(n, side).wait_recv()
                r = 128 * side
                decode_sum(chunk, r, 0, chunk, r, 0, 128, width, [(rA.at[side], 0)])
                encode(chunk, (r,), 128, 0, width, sB.at[side, side])
                B_second(n, side, side).start()

    dims = (((0,), (0,)), ((), ()))

    def start_group(i):
        j, k = lax.div(i, 4), rem4(i)
        a = acc.at[lax.rem(i, SLOTS)]
        need, have = pick(i, NEED), pick(i, HAVE)
        for t in range(2):

            @pl.when(need > t)
            def _():
                local_tok(have + t).wait()
                remote_tok(have + t).wait_recv()

        x, z = place(k, j)
        x2, z2 = place(j, k)
        cols = pl.ds(row0(x, z), 256)
        cols2 = pl.ds(row0(x2, z2), 256)
        a[:, :C2] = lax.dot_general(
            tok[0, :, cols], w[0, :, :C2], dims, preferred_element_type=jnp.float32
        ) + lax.dot_general(tok[1, :, cols], w[1, :, :C2], dims, preferred_element_type=jnp.float32)
        a[:, C2:] = lax.dot_general(
            tok[0, :, cols2], w[0, :, C2:], dims, preferred_element_type=jnp.float32
        ) + lax.dot_general(tok[1, :, cols2], w[1, :, C2:], dims, preferred_element_type=jnp.float32)
        g = x * 4 + z
        y1, y2, y3 = (pl.multiple_of(rem4(Y + d) * 64, 64) for d in (1, 2, 3))
        encode(a, (y2, y1 + 32), 32, C1, W1, sA1.at[g, 0])
        encode(a, (y2 + 32, y3), 32, C1, W1, sA1.at[g, 1])
        for side in range(2):
            A1(g, side).start()

        @pl.when(k == 0)
        def _():
            for side in range(2):
                encode(a, (128 * side,), 128, C0, W0, sA0.at[z, side])
                encode(a, (128 * side,), 128, C2, W2, sA2.at[x2, side])
            for side in range(2):
                A0(z, side).start()
                A2(x2, side).start()

        for side in range(2):

            @pl.when(k == 1 + side)
            def _():
                r = 128 * (1 - side)
                encode(a, (r,), 128, C0, W0, sB0.at[z, side, 1 - side])
                encode(a, (r,), 128, C2, W2, sB2.at[x2, side, 1 - side])
                B0(z, side, 1 - side).start()
                B2(x2, side, 1 - side).start()

    def send_group(i):
        j, k = lax.div(i, 4), rem4(i)
        a = acc.at[lax.rem(i, SLOTS)]
        x, z = place(k, j)
        x2, z2 = place(j, k)
        g = x * 4 + z
        for side in range(2):
            A1(g, side).wait_recv()
        for side in range(2):
            r = pl.multiple_of(rem4(Y + 1 + 2 * side) * 64, 64) + 32 * side
            decode_sum(a, r, C1, a, r, C1, 32, W1, [(rA1.at[g, side], 0)])
            encode(a, (r,), 32, C1, W1, sB1.at[g, side])
        for side in range(2):
            B1(g, side).start()
        for side in range(2):

            @pl.when(k == 1 + side)
            def _():
                r = 128 * side
                A0(z, side).wait_recv()
                A2(x2, side).wait_recv()
                decode_sum(a, r, C0, a, r, C0, 128, W0, [(rA0.at[z, side], 0)])
                encode(a, (r,), 128, C0, W0, sB0.at[z, side, side])
                decode_sum(a, r, C2, a, r, C2, 128, W2, [(rA2.at[x2, side], 0)])
                encode(a, (r,), 128, C2, W2, sB2.at[x2, side, side])
                B0(z, side, side).start()
                B2(x2, side, side).start()

    def sum_group(i):
        j, k = lax.div(i, 4), rem4(i)
        a = acc.at[lax.rem(i, SLOTS)]
        x, z = place(k, j)
        x2, z2 = place(j, k)
        g = x * 4 + z
        both(sB1, rB1, b1_s, b1_r, g).wait_recv()
        mine = pl.multiple_of(Y * 64, 64)
        x64 = pl.multiple_of(x * 64, 64)
        for h in range(2):
            parts = [(rB1.at[g, h], 0), (rA1.at[g, 1 - h], tiles(32, W1))]
            decode_sum(own1.at[z], x64 + 32 * h, 0, a, mine + 32 * h, C1, 32, W1, parts)

        @pl.when(k == 3)
        def _():
            both(sB0, rB0, b0_s, b0_r, z).wait_recv()
            for h in range(2):
                r = 128 * h
                decode_sum(own0.at[z], r, 0, a, r, C0, 128, W0, [(rB0.at[z, 0, h], 0), (rB0.at[z, 1, h], 0)])
            second_phase(0, z, j)
            second_phase(1, z, j)
            both(sB2, rB2, b2_s, b2_r, x2).wait_recv()
            for h in range(2):
                r = 128 * h
                decode_sum(own2.at[x2], r, 0, a, r, C2, 128, W2, [(rB2.at[x2, 0, h], 0), (rB2.at[x2, 1, h], 0)])
            second_phase(2, x2, j)

    def step(i, carry):
        @pl.when(i < 16)
        def _():
            start_group(i)

        @pl.when((i >= LAG_B) & (i < 16 + LAG_B))
        def _():
            send_group(i - LAG_B)

        @pl.when(i >= LAG_SUM)
        def _():
            sum_group(i - LAG_SUM)

        return carry

    lax.fori_loop(0, 16 + LAG_SUM, step, 0)

    def ring_y(d):
        return dev(X, rem4(Y + d), Z, C)

    def ring_x(d):
        return dev(rem4(X + d), Y, Z, C)

    third_rings = (
        (own0.at[Z], W0, Y, s3.at[0], r3.at[0], ring_y),
        (own1.at[Z], W1, X, s3.at[1], r3.at[1], ring_x),
        (own2.at[X], W2, Y, s32, r32, ring_y),
    )

    def third(n, d):
        own, width, at, S, R, to = third_rings[n]
        return remote(S.at[d - 1], R.at[d - 1], p3_s.at[n], p3_r.at[n], to(d))

    for n, m in ((0, Z), (1, Z), (2, X)):
        own, width, sA, rA, sB, rB, plus, minus = second_rings[n]
        remote(sB, rB, p2b_s.at[n], p2b_r.at[n], partner).wait_recv()
        for h in range(2):
            r = 128 * h
            decode_sum(own.at[m], r, 0, own.at[m], r, 0, 128, width, [(rB.at[0, h], 0), (rB.at[1, h], 0)])
        own, width, at, S, R, to = third_rings[n]
        for d in (2, 1, 3):
            encode(own, (pl.multiple_of(rem4(at + d) * 64, 64),), 64, 0, width, S.at[d - 1])
        for d in (2, 1, 3):
            third(n, d).start()
    col = 0
    square = jnp.zeros((8, 128), jnp.float32)
    for n, (own, width, at, S, R, to) in enumerate(third_rings):
        r = pl.multiple_of(at * 64, 64)
        remote(S, R, p3_s.at[n], p3_r.at[n], partner).wait_recv()
        decode_sum(own, r, 0, own, r, 0, 64, width, [(R.at[d], 0) for d in range(3)])
        for t in range(8):
            for j in range(width // 128):
                v = own[pl.ds(r + t * 8, 8), pl.ds(j * 128, 128)]
                fin[pl.ds(t * 8, 8), pl.ds(col + j * 128, 128)] = v
                square = square + v * v
        col += width

    nrm1[here] = jnp.sum(square, axis=0, keepdims=True)
    exchange(nrm1, here, 8, near, none_s, none_r)
    theirs = pl.ds(pl.multiple_of((1 - C) * 32, 32), 32)
    mine = pl.ds(pl.multiple_of(C * 32, 32), 32)
    swap = remote(fin.at[theirs], finr, f_s, f_r, partner)
    swap.start()
    everything(nrm1, 8, none_s, none_r).wait_recv()
    nrm2[plane] = total_of(nrm1, 8)
    exchange(nrm2, plane, 16, far, ntwo_s, ntwo_r)

    for S, ss in ((sA0, a0_s), (sB0, b0_s), (sA1, a1_s), (sB1, b1_s), (sA2, a2_s), (sB2, b2_s)):
        remote(S, S, ss, f_r, partner).wait_send()
    for n in range(3):
        own, width, sA, rA, sB, rB, plus, minus = second_rings[n]
        remote(sA, rA, p2a_s.at[n], f_r, partner).wait_send()
        remote(sB, rB, p2b_s.at[n], f_r, partner).wait_send()
        own, width, at, S, R, to = third_rings[n]
        remote(S, R, p3_s.at[n], f_r, partner).wait_send()
    remote(tok_hbm, tok.at[1], tok_s, f_r, partner).wait_send()
    in_cot.wait_send()
    in_idx.wait_send()
    for slots, count, ss in ((cnt1, 8, one_s), (cnt2, 16, two_s), (nrm1, 8, none_s), (nrm2, 16, ntwo_s)):
        everything(slots, count, ss, f_r).wait_send()
    swap.wait()
    everything(nrm2, 16, ntwo_s, ntwo_r).wait_recv()
    square = total_of(nrm2, 16)
    root_mean = jnp.sqrt(jnp.sum(square, keepdims=True) / (D * QW))
    factor = 1.0 / jnp.maximum(root_mean, 1.0)
    grad_ref[:, my_cols] = fin[mine, :] * factor
    grad_ref[:, other_cols] = finr[...] * factor


def shards(tokens_in, query_cotangent, task_index, loss_weights, master, moment_first, moment_second):
    i16 = jnp.int16

    def msgs(lead, rows, width):
        return pltpu.VMEM((*lead, tiles(rows, width) + 1, 16, 128), i16)

    f32 = jnp.float32
    dma = pltpu.SemaphoreType.DMA
    scratch = [
        pltpu.SMEM((TASKS,), jnp.int32),
        pltpu.VMEM((2, TOK, D), jnp.bfloat16),
        pltpu.VMEM((2, TOK, HALF), jnp.bfloat16),
        pltpu.VMEM((2, 8, 128), jnp.int32),
        pltpu.VMEM((2, 8, 128), f32),
        pltpu.VMEM((SLOTS, 256, HALF), f32),
        pltpu.VMEM((4, 256, W0), f32),
        pltpu.VMEM((4, 256, W1), f32),
        pltpu.VMEM((4, 256, W2), f32),
        msgs((4, 2), 128, W0), msgs((4, 2), 128, W0), msgs((4, 2, 2), 128, W0), msgs((4, 2, 2), 128, W0),
        msgs((4, 2), 128, W2), msgs((4, 2), 128, W2), msgs((4, 2, 2), 128, W2), msgs((4, 2, 2), 128, W2),
        msgs((16, 2), 64, W1), msgs((16, 2), 64, W1), msgs((16, 2), 32, W1), msgs((16, 2), 32, W1),
        msgs((2, 2), 128, W0), msgs((2, 2), 128, W0), msgs((2, 2, 2), 128, W0), msgs((2, 2, 2), 128, W0),
        msgs((2,), 128, W2), msgs((2,), 128, W2), msgs((2, 2), 128, W2), msgs((2, 2), 128, W2),
        msgs((2, 3), 64, W0), msgs((2, 3), 64, W0), msgs((3,), 64, W2), msgs((3,), 64, W2),
        pltpu.VMEM((8, 1, 128), jnp.int32),
        pltpu.VMEM((16, 1, 128), jnp.int32),
        pltpu.VMEM((8, 1, 128), f32),
        pltpu.VMEM((16, 1, 128), f32),
        pltpu.VMEM((64, HALF), f32),
        pltpu.VMEM((32, HALF), f32),
        dma((19,)), dma(()), dma((16,)), dma((2,)), dma((2,)),
        dma(()), dma(()), dma(()), dma(()), dma(()), dma(()), dma(()), dma(()),
        dma(()), dma((4, 2)), dma(()), dma((4,)),
        dma(()), dma((16, 2)), dma(()), dma((16,)),
        dma(()), dma((4, 2)), dma(()), dma((4,)),
        dma((3,)), dma((3, 2)), dma((3,)), dma((3,)), dma((3,)), dma((3,)),
        dma(()), dma(()),
    ]
    hbm = pl.BlockSpec(memory_space=pl.ANY)
    vmem = pl.BlockSpec(memory_space=pltpu.VMEM)
    clipped = pl.pallas_call(
        kernel,
        out_shape=jax.ShapeDtypeStruct((32, QW), f32),
        in_specs=[hbm] * 4,
        out_specs=vmem,
        scratch_shapes=scratch,
        compiler_params=pltpu.CompilerParams(
            collective_id=0, has_side_effects=True, vmem_limit_bytes=62 * 1024 * 1024
        ),
    )(tokens_in, query_cotangent, task_index.reshape(8, 128), loss_weights)
    new_first = beta_one * moment_first + (1.0 - beta_one) * clipped
    new_second = beta_two * moment_second + (1.0 - beta_two) * clipped * clipped
    direction = new_first / corr_one / (jnp.sqrt(new_second / corr_two) + adam_eps)
    new_master = master - step_rate * (direction + decay_rate * master)
    return (new_master, new_first, new_second)


def solution(mesh):
    finer = Mesh(mesh.devices.reshape(2, 4, 2, 4, 2), AXES)
    rows = P(AXES, None)
    in_specs = (rows, rows, P(AXES), P(), rows, rows, rows)
    return jax.shard_map(
        shards, mesh=finer, in_specs=in_specs, out_specs=(rows, rows, rows), check_vma=False
    )
```
